128 devices in a mesh: trade: 8 (over y, core), scen: 16 (over z, x).
Axes of the slice: x: 4, y: 4, z: 4, core: 2. Of those that a mesh axis runs over, the one named last changes fastest.
Arguments:
- factors: float32 [4096, 64], P('scen'), may hold values from -1 to 1
- feat_factor: int32 [1024], replicated, may hold values from 0 to 63
- feat_degree: int32 [1024], replicated, may hold values from 1 to 12
- coefficients: float32 [1024, 16384], P(None, 'trade'), may hold values from -0.1875 to 0.1875
- set_of_trade: int32 [16384], P('trade'), may hold values from 0 to 1023, as said below
- party_of_set: int32 [1024], P('trade'), may hold values from 0 to 1023
- threshold: float32 [1024], replicated, may hold values from 0 to 4
- weight: float32 [1024], replicated, may hold values from 0.5 to 2
Outputs:
- xva: float32 [1024], P('trade')
- coef_sens: float32 [1024, 16384], P('scen', 'trade')
- feature_sens: float32 [1024, 4096], P('trade', 'scen')
The draws below stay inside these ranges and needn't reach their ends.
Inputs may be any that keep to these rules, and one draw needn't show every extreme that they name: `set_of_trade`: each netting set holds exactly 16 trades; the trades of aligned block b of 2048 trades belong to sets b * 128 to (b + 1) * 128 - 1.
All inputs are finite; a program needn't handle non-finite values.
Results may differ from the reference program's by a relative error of at most 0.000073.
Values sent between devices are 32-bit elements; how exact they have to be, the bound alone decides.
A program may use at most 64 MiB of HBM per device.

```python
import math
import jax
import jax.numpy as jnp
import numpy as np
from jax import lax

K = 1024
NFAC = 64
MAXDEG = 12
SET_SIZE = 16
TR_DEV = 2048
TRADES = 16384
SCEN = 4096
NSETS = 1024
NCP = 1024


def draw_set_of_trade(key, part):
    blocks = TRADES // TR_DEV
    keys = jax.random.split(jax.random.fold_in(key, 11), blocks)
    orders = jax.vmap(lambda single: jax.random.permutation(single, TR_DEV))(keys)
    offsets = jnp.arange(blocks, dtype=jnp.int32) * (TR_DEV // SET_SIZE)
    sets = orders.astype(jnp.int32) // SET_SIZE + offsets[:, None]
    return sets.reshape(TRADES).astype(jnp.int32)


def with_ends(values, own_key, low, high):
    spot = [jax.random.randint(jax.random.fold_in(own_key, axis), (), 0, length) for axis, length in enumerate(values.shape)]
    widest = values.shape.index(max(values.shape))
    next_to = spot[:widest] + [(spot[widest] + 1) % values.shape[widest]] + spot[widest + 1:]
    return values.at[tuple(spot)].set(low).at[tuple(next_to)].set(high)


def steps_of(key, dims, shards, smallest, high):
    level, own = 1.0, jax.random.fold_in(key, 6)
    for position, blocks in shards:
        draws = jnp.exp(jax.random.uniform(jax.random.fold_in(own, position), (blocks,), jnp.float32, smallest / len(shards), high / len(shards)))
        level = level * jnp.repeat(draws, dims[position] // blocks).reshape([-1 if axis == position else 1 for axis in range(len(dims))])
    return level


def rank_table(number_of, slope):
    portions = [(1 << 20) // math.isqrt(standing ** slope) + 1 for standing in range(1, number_of + 1)]
    scale = 1 + sum(portions) // (1 << 30)
    return np.cumsum(np.array([max(1, weight // scale) for weight in portions]))


def ranked_ids(own_key, dims, count, slope):
    grid = rank_table(count, slope)
    ticket = jax.random.randint(jax.random.fold_in(own_key, 1), dims, 0, int(grid[count - 1]))
    grade = jnp.searchsorted(jnp.asarray(grid, jnp.int32), ticket, side="right")
    return jax.random.permutation(jax.random.fold_in(own_key, 2), count)[grade].astype(jnp.int32)


def scatter_about(stream_key, dims, deviation, reach, shards=(), kind=jnp.bfloat16):
    array = jax.random.normal(stream_key, dims, jnp.float32) * deviation
    if len(shards) > 0:
        array = steps_of(stream_key, dims, shards, -0.22, 0.18) * array
    return jnp.clip(array, min=-reach, max=reach).astype(kind)


def setup_inputs(seed: int = 0) -> dict:
    key_of = jax.random.split(jax.random.key(seed), 9)
    return {
        "factors": jnp.clip(jax.random.uniform(key_of[0], (SCEN, NFAC), jnp.float32, -1.0, 1.0) * steps_of(key_of[0], (SCEN, NFAC), ((0, 16),), -0.4, 0.0), -1.0, 1.0),
        "feat_factor": with_ends(jax.random.randint(key_of[1], (K,), 0, NFAC), jax.random.fold_in(key_of[1], 1), 0, NFAC - 1).astype(jnp.int32),
        "feat_degree": with_ends(jax.random.randint(key_of[2], (K,), 1, MAXDEG + 1), jax.random.fold_in(key_of[2], 1), 1, MAXDEG).astype(jnp.int32),
        "coefficients": scatter_about(key_of[3], (K, TRADES), K ** -0.5, 0.1875, ((1, 8),), jnp.float32),
        "set_of_trade": draw_set_of_trade(jax.random.fold_in(key_of[8], 71), 0),
        "party_of_set": with_ends(ranked_ids(key_of[5], (NSETS,), NCP, 2), jax.random.fold_in(key_of[5], 3), 0, NCP - 1).astype(jnp.int32),
        "threshold": jnp.clip(jax.random.uniform(key_of[6], (NCP,), jnp.float32, 0.0, 4.0), 0.0, 4.0),
        "weight": jnp.clip(jnp.exp(jax.random.uniform(key_of[7], (NCP,), jnp.float32, math.log(0.5), math.log(2.0))), 0.5, 2.0),
    }


highest = lax.Precision.HIGHEST


def chebyshev(points, degrees):
    before = jnp.ones_like(points)
    current = points
    result = jnp.where(degrees[None, :] == 1, current, jnp.zeros_like(points))
    for order in range(2, MAXDEG + 1):
        before, current = current, 2.0 * points * current - before
        result = jnp.where(degrees[None, :] == order, current, result)
    return result


def reference(factors, feat_factor, feat_degree, coefficients, set_of_trade, party_of_set, threshold, weight):
    points = factors[:, feat_factor]
    phi = chebyshev(points, feat_degree)
    folded = jax.ops.segment_sum(coefficients.T, set_of_trade, NSETS).T
    exposure = jnp.dot(phi, folded, precision=highest)
    netted = jax.ops.segment_sum(exposure.T, party_of_set, NCP).T
    shifted = netted - threshold[None, :]
    xva = weight * jnp.sum(jax.nn.softplus(shifted), axis=0) / SCEN
    party_adj = weight[None, :] * jax.nn.sigmoid(shifted)
    set_adj = party_adj[:, party_of_set]
    set_grad = jnp.dot(phi.T, set_adj, precision=highest) / SCEN
    coef_sens = set_grad[:, set_of_trade]
    feature_sens = jnp.dot(folded, set_adj.T, precision=highest)
    return xva, coef_sens, feature_sens
```

```python
import jax
import jax.numpy as jnp
from jax import lax
from jax.experimental import pallas as pl
from jax.experimental.pallas import tpu as pltpu
from jax.sharding import PartitionSpec as P

MAXDEG = 12
SCEN = 4096
MESH = pl.DeviceIdType.MESH
BF = jnp.bfloat16
F32 = jnp.float32


def mm(left, right):
    return lax.dot_general(left, right, (((1,), (0,)), ((), ())), preferred_element_type=F32)


def mm_nt(left, right):
    return lax.dot_general(left, right, (((1,), (1,)), ((), ())), preferred_element_type=F32)


def halves(value):
    high = value.astype(BF)
    return high, (value - high.astype(F32)).astype(BF)


def thirds(value):
    high = value.astype(BF)
    rest = value - high.astype(F32)
    mid = rest.astype(BF)
    return high, mid, (rest - mid.astype(F32)).astype(BF)


def iota(shape, dim):
    return lax.broadcasted_iota(jnp.int32, shape, dim)


def onehot(mask):
    return jnp.where(mask, 1.0, 0.0).astype(BF)


def upright(row):
    return jnp.broadcast_to(row, (128, 128)).T


def chebyshev_split(points, degrees):
    before = jnp.ones_like(points)
    current = points
    result = jnp.where(degrees == 1, points, 0.0)
    twice = points + points
    for order in range(2, MAXDEG + 1):
        before, current = current, twice * current - before
        result = jnp.where(degrees == order, current, result)
    return halves(result)


def kernel(
    coef_hbm, fac_ref, ff_ref, fd_ref, sot_ref, pos_ref, thr_ref, w_ref,
    xva_out, coef_out, feat_out,
    cbuf, member, memt, pts, phi_h, phi_l, fax, faz, pha_h, pha_l, phb_h, phb_l,
    folded, frows, etb, eh, ehl, party, pcol, same, ownp, tw, sas, sa, sb, sat,
    xs, xr, xt, xz, ga, gb, gra, grb, cst, fst, xst,
    c_sem, p_snd, p_rcv, fx_snd, fx_rcv, fz_snd, fz_rcv, e_snd, e_rcv, f_snd, f_rcv,
    sa_snd, sa_rcv, sb_snd, sb_rcv, st_snd, st_rcv, x_snd, x_rcv, x2_snd, x2_rcv,
    ga_snd, ga_rcv, gb_snd, gb_rcv, o_sem,
):
    t = lax.axis_index("trade")
    sigma = lax.axis_index("scen")
    y, c = t // 2, t % 2
    z, x = sigma // 4, sigma % 4

    def remote(src, dst, snd, rcv, trade, scen):
        return pltpu.make_async_remote_copy(
            src_ref=src, dst_ref=dst, send_sem=snd, recv_sem=rcv,
            device_id=(trade, scen), device_id_type=MESH,
        )

    def tr(k):
        return lax.rem(t + k, 8)

    def xpeer(k):
        return z * 4 + lax.rem(x + k, 4)

    def zpeer(k):
        return lax.rem(z + k, 4) * 4 + x

    loads = []
    for i in range(8):
        rows = pl.ds(128 * i, 128)
        load = pltpu.make_async_copy(coef_hbm.at[rows], cbuf.at[rows], c_sem.at[i])
        load.start()
        loads.append(load)

    barrier = pltpu.get_barrier_semaphore()
    for k in range(1, 8):
        pl.semaphore_signal(barrier, inc=1, device_id=(tr(k), sigma), device_id_type=MESH)
    for k in range(1, 4):
        for d in range(2):
            pl.semaphore_signal(barrier, inc=1, device_id=(2 * y + d, xpeer(k)), device_id_type=MESH)
            pl.semaphore_signal(barrier, inc=1, device_id=(2 * y + d, zpeer(k)), device_id_type=MESH)

    packed = jnp.concatenate([fac_ref[0:128, :], fac_ref[128:256, :]], axis=1)
    fax[x] = packed
    faz[z] = packed

    base = (128 * t).astype(F32)
    lanes = iota((128, 128), 1).astype(F32)
    for j in range(16):
        col = upright(sot_ref[:, 128 * j:128 * j + 128].astype(F32) - base)
        member[128 * j:128 * j + 128, :] = onehot(col == lanes)

    def lookup3(ff, cols, half):
        one = onehot(iota((128, cols), 0) == ff + 64 * half)
        return jnp.concatenate([one, one, one], axis=0)

    three = jnp.concatenate(thirds(packed), axis=1)
    for half in range(2):
        pts[128 * half:128 * half + 128, :] = mm(three, lookup3(ff_ref[...], 1024, half))

    def cheb_own(i, carry):
        cols = pl.ds(pl.multiple_of((i // 4) * 128, 128), 128)
        rows = pl.ds(pl.multiple_of((i % 4) * 64, 64), 64)
        high, low = chebyshev_split(pts[rows, cols], fd_ref[:, cols])
        phi_h[rows, cols] = high
        phi_l[rows, cols] = low
        return carry

    lax.fori_loop(0, 32, cheb_own, 0)

    pl.semaphore_wait(barrier, 19)

    party_sends = []
    for k in range(1, 8):
        send = remote(pos_ref, party.at[t], p_snd.at[k - 1], p_rcv.at[t], tr(k), sigma)
        send.start()
        party_sends.append(send)
    fac_sends = []
    for k in range(1, 4):
        send = remote(fax.at[x], fax.at[x], fx_snd.at[k - 1], fx_rcv.at[x], t, xpeer(k))
        send.start()
        fac_sends.append(send)
        send = remote(faz.at[z], faz.at[z], fz_snd.at[k - 1], fz_rcv.at[z], t, zpeer(k))
        send.start()
        fac_sends.append(send)
    party[t] = pos_ref[...]

    for i in range(8):
        loads[i].wait()
        rows = slice(128 * i, 128 * i + 128)
        high, low = halves(cbuf[rows, :])
        folded[i] = mm(high, member[...]) + mm(low, member[...])
    exposure = jnp.zeros((256, 128), F32)
    for i in range(8):
        cols = slice(128 * i, 128 * i + 128)
        high, low = halves(folded[i])
        wide = mm(phi_h[:, cols], jnp.concatenate([high, low], axis=1))
        exposure = exposure + wide[:, :128] + wide[:, 128:] + mm(phi_l[:, cols], high)
    etb[0] = exposure[0:128, :].T
    etb[1] = exposure[128:256, :].T

    e_sends = []
    for k in (4, 5, 3, 2, 6, 7, 1):
        other = tr(k)
        send = remote(etb.at[other % 2], eh.at[t], e_snd.at[k - 1], e_rcv.at[t], other, sigma)
        send.start()
        e_sends.append(send)
    f_sends = []
    for k in (4, 5, 3, 2, 6, 7, 1):
        other = tr(k)
        send = remote(folded.at[other], frows.at[t], f_snd.at[k - 1], f_rcv.at[t], other, sigma)
        send.start()
        f_sends.append(send)
    eh[t] = etb[c]
    frows[t] = folded[t]

    for k in range(1, 8):
        src = tr(k)
        remote(pos_ref, party.at[src], p_snd.at[k - 1], p_rcv.at[src], src, sigma).wait_recv()
    for j in range(8):
        pcol[j] = upright(party[j].astype(F32))
    table = thirds(thr_ref[...]) + thirds(w_ref[...])
    table = jnp.concatenate([part.astype(F32) for part in table] + [jnp.zeros((2, 1024), F32)], axis=0).astype(BF)

    def rows_of(j, carry):
        col = pcol[j]
        rows = pl.ds(pl.multiple_of(j * 128, 128), 128)
        for i in range(8):
            same[rows, 128 * i:128 * i + 128] = onehot(col == party[i].astype(F32))
        spread = jnp.concatenate([onehot(col == lanes + 128.0 * i) for i in range(8)], axis=1)
        tw[j] = mm_nt(spread, table)
        return carry

    lax.fori_loop(0, 8, rows_of, 0)
    for i in range(8):
        ownp[:, 128 * i:128 * i + 128] = onehot(iota((256, 128), 0) + 256 * y == party[i])

    fvals = jnp.concatenate([ff_ref[...].astype(F32), fd_ref[...].astype(F32), jnp.zeros((6, 1024), F32)], axis=0).astype(BF)
    lane256 = iota((1024, 256), 1)
    fidx_a = ((lane256 // 64) * 4 + x) * 64 + lane256 % 64
    fidx_b = z * 256 + lane256
    picks = []
    for fidx in (fidx_a, fidx_b):
        picked = mm(fvals, onehot(iota((1024, 256), 0) == fidx)).astype(jnp.int32)
        picks.append((picked[0:1, :], picked[1:2, :]))

    def phi_of(buf, ff, fd, out_h, out_l):
        for half in range(2):
            look = lookup3(ff, 256, half)
            for q in range(4):
                pts[0:128, 256 * q:256 * q + 256] = mm(jnp.concatenate(thirds(buf[q]), axis=1), look)
            for q in range(4):
                for b in range(2):
                    def cheb(r, carry, q=q, b=b):
                        rows = pl.ds(pl.multiple_of(r * 64, 64), 64)
                        high, low = chebyshev_split(
                            pts[rows, 256 * q + 128 * b:256 * q + 128 * b + 128], fd[:, 128 * b:128 * b + 128]
                        )
                        out_h[2 * q + half, rows, 128 * b:128 * b + 128] = high
                        out_l[2 * q + half, rows, 128 * b:128 * b + 128] = low
                        return carry

                    lax.fori_loop(0, 2, cheb, 0)

    for k in range(1, 4):
        src = lax.rem(x + k, 4)
        remote(fax.at[x], fax.at[src], fx_snd.at[k - 1], fx_rcv.at[src], t, xpeer(k)).wait_recv()
    phi_of(fax, picks[0][0], picks[0][1], pha_h, pha_l)
    for k in range(1, 4):
        src = lax.rem(z + k, 4)
        remote(faz.at[z], faz.at[src], fz_snd.at[k - 1], fz_rcv.at[src], t, zpeer(k)).wait_recv()
    phi_of(faz, picks[1][0], picks[1][1], phb_h, phb_l)

    for k in range(1, 8):
        src = tr(k)
        remote(etb.at[0], eh.at[src], e_snd.at[k - 1], e_rcv.at[src], src, sigma).wait_recv()
    for j in range(8):
        high, low = halves(eh[j])
        ehl[128 * j:128 * j + 128, 0:128] = high
        ehl[128 * j:128 * j + 128, 128:256] = low

    def adjoint(j):
        rows = pl.ds(pl.multiple_of(j * 128, 128), 128)
        wide = mm(same[rows, :], ehl[...])
        consts = tw[j]
        shift = consts[:, 0:1] + consts[:, 1:2] + consts[:, 2:3]
        scale = consts[:, 3:4] + consts[:, 4:5] + consts[:, 5:6]
        return scale * jax.nn.sigmoid(wide[:, :128] + wide[:, 128:] - shift)

    for d in range(2):
        sas[d] = adjoint(2 * y + d)
    s_sends = []
    for k in range(0, 4):
        for e in range(2):
            if k == 0 and e == 0:
                continue
            d = lax.rem(c + e, 2)
            i = 2 * k + e - 1
            send = remote(sas.at[d, pl.ds(0, 64)], sa.at[2 * x + c], sa_snd.at[i], sa_rcv.at[2 * x + c], 2 * y + d, xpeer(k))
            send.start()
            s_sends.append(send)
            send = remote(sas.at[d, pl.ds(64, 64)], sb.at[2 * z + c], sb_snd.at[i], sb_rcv.at[2 * z + c], 2 * y + d, zpeer(k))
            send.start()
            s_sends.append(send)
    sa[2 * x + c] = sas[c, 0:64, :]
    sb[2 * z + c] = sas[c, 64:128, :]

    def other_rows(j, carry):
        sat[c, j] = adjoint(j)
        return carry

    lax.fori_loop(0, 8, other_rows, 0)
    partner = 2 * y + 1 - c
    sat_send = remote(sat.at[c], sat.at[c], st_snd, st_rcv, partner, sigma)
    sat_send.start()

    wide = mm(ownp[...], ehl[...])
    for d in range(2):
        first = pl.multiple_of(256 * y + 128 * d, 128)
        limit = upright(thr_ref[:, pl.ds(first, 128)])
        soft = jax.nn.softplus(wide[128 * d:128 * d + 128, :128] + wide[128 * d:128 * d + 128, 128:] - limit)
        xs[d] = jnp.broadcast_to(jnp.sum(soft.T, axis=0, keepdims=True), (8, 128))
    x_sends = []
    for k in range(0, 4):
        for e in range(2):
            if k == 0 and e == 0:
                continue
            d = lax.rem(c + e, 2)
            send = remote(xs.at[d], xr.at[2 * x + c], x_snd.at[2 * k + e - 1], x_rcv.at[2 * x + c], 2 * y + d, xpeer(k))
            send.start()
            x_sends.append(send)
    xr[2 * x + c] = xs[c]

    for k in range(1, 8):
        src = tr(k)
        remote(folded.at[0], frows.at[src], f_snd.at[k - 1], f_rcv.at[src], src, sigma).wait_recv()
    remote(sat.at[c], sat.at[1 - c], st_snd, st_rcv, partner, sigma).wait_recv()
    sums = [jnp.zeros((128, 128), F32) for _ in range(2)]
    for j in range(8):
        left_h, left_l = halves(frows[j])
        for d in range(2):
            high, low = halves(sat[d, j])
            sums[d] = sums[d] + mm(left_h, high) + mm(left_h, low) + mm(left_l, high)
    fst[:, 0:128] = sums[0]
    fst[:, 128:256] = sums[1]
    feat_copy = pltpu.make_async_copy(fst, feat_out, o_sem.at[0])
    feat_copy.start()

    low_lanes = iota((32, 128), 1) < 64

    def gradient(slots, out_h, out_l, dest):
        total = jnp.zeros((64, 256), F32)
        for j in range(8):
            high, low = halves(slots[j])
            total = total + mm(high, out_h[j]) + mm(low, out_h[j]) + mm(high, out_l[j])
        for pair in range(2):
            top = total[0:32, 128 * pair:128 * pair + 128]
            bottom = total[32:64, 128 * pair:128 * pair + 128]
            dest[2 * pair] = jnp.where(low_lanes, top, pltpu.roll(bottom, 64, 1))
            dest[2 * pair + 1] = jnp.where(low_lanes, pltpu.roll(top, 64, 1), bottom)

    def wait_slots(buf, rcv, snd, mine, peer):
        for k in range(0, 4):
            for e in range(2):
                if k == 0 and e == 0:
                    continue
                d = lax.rem(c + e, 2)
                slot = 2 * lax.rem(mine + k, 4) + d
                remote(buf.at[slot], buf.at[slot], snd.at[2 * k + e - 1], rcv.at[slot], 2 * y + d, peer(k)).wait_recv()

    g_sends = []
    wait_slots(sa, sa_rcv, sa_snd, x, xpeer)
    gradient(sa, pha_h, pha_l, ga)
    for k in (2, 1, 3):
        send = remote(ga.at[lax.rem(z + k, 4)], gra.at[z], ga_snd.at[k - 1], ga_rcv.at[z], t, zpeer(k))
        send.start()
        g_sends.append(send)
    wait_slots(sb, sb_rcv, sb_snd, z, zpeer)
    gradient(sb, phb_h, phb_l, gb)
    for k in (2, 1, 3):
        send = remote(gb.at[lax.rem(x + k, 4)], grb.at[x], gb_snd.at[k - 1], gb_rcv.at[x], t, xpeer(k))
        send.start()
        g_sends.append(send)
    gra[z] = ga[z]
    grb[x] = gb[x]

    wait_slots(xr, x_rcv, x_snd, x, xpeer)
    part = xr[0]
    for j in range(1, 8):
        part = part + xr[j]
    xt[...] = part
    for k in range(1, 4):
        send = remote(xt, xz.at[z], x2_snd.at[k - 1], x2_rcv.at[z], t, zpeer(k))
        send.start()
        x_sends.append(send)
    xz[z] = part

    row = iota((128, 128), 0)
    of_row = (row // 64) * 32 + ((row % 64) // 32) * 64 + row % 32 + 128 * t
    for j in range(16):
        memt[:, 128 * j:128 * j + 128] = onehot(of_row == sot_ref[:, 128 * j:128 * j + 128])

    for k in range(1, 4):
        src = lax.rem(z + k, 4)
        remote(ga.at[0], gra.at[src], ga_snd.at[k - 1], ga_rcv.at[src], t, zpeer(k)).wait_recv()
    for k in range(1, 4):
        src = lax.rem(x + k, 4)
        remote(gb.at[0], grb.at[src], gb_snd.at[k - 1], gb_rcv.at[src], t, xpeer(k)).wait_recv()
    grad_a = (gra[0] + gra[1]) + (gra[2] + gra[3])
    grad_b = (grb[0] + grb[1]) + (grb[2] + grb[3])
    grads = (jnp.concatenate([grad_a, grad_b], axis=0) * (1.0 / SCEN)).T
    high, low = halves(grads)
    even, odd = memt[0:64, :], memt[64:128, :]
    cst[...] = (mm(high[0:64], even) + mm(low[0:64], even)) + (mm(high[64:128], odd) + mm(low[64:128], odd))
    coef_copy = pltpu.make_async_copy(cst, coef_out, o_sem.at[1])
    coef_copy.start()

    for k in range(1, 4):
        src = lax.rem(z + k, 4)
        remote(xt, xz.at[src], x2_snd.at[k - 1], x2_rcv.at[src], t, zpeer(k)).wait_recv()
    whole = (xz[0] + xz[1]) + (xz[2] + xz[3])
    first = pl.multiple_of(128 * t, 128)
    xst[...] = w_ref[:, pl.ds(first, 128)] * whole[0:1, :] * (1.0 / SCEN)
    xva_copy = pltpu.make_async_copy(xst, xva_out, o_sem.at[2])
    xva_copy.start()

    for send in party_sends + fac_sends + e_sends + f_sends + s_sends + [sat_send] + x_sends + g_sends:
        send.wait_send()
    feat_copy.wait()
    coef_copy.wait()
    xva_copy.wait()


def local(factors, feat_factor, feat_degree, coefficients, set_of_trade, party_of_set, threshold, weight):
    vmem = pl.BlockSpec(memory_space=pltpu.VMEM)
    anywhere = pl.BlockSpec(memory_space=pl.ANY)
    V = pltpu.VMEM
    D = pltpu.SemaphoreType.DMA
    scratch = [
        V((1024, 2048), F32),
        V((2048, 128), BF),
        V((128, 2048), BF),
        V((256, 1024), F32),
        V((256, 1024), BF), V((256, 1024), BF),
        V((4, 128, 128), F32), V((4, 128, 128), F32),
        V((8, 128, 256), BF), V((8, 128, 256), BF), V((8, 128, 256), BF), V((8, 128, 256), BF),
        V((8, 128, 128), F32),
        V((8, 128, 128), F32),
        V((2, 128, 128), F32),
        V((8, 128, 128), F32),
        V((1024, 256), BF),
        V((8, 1, 128), jnp.int32),
        V((8, 128, 128), F32),
        V((1024, 1024), BF),
        V((256, 1024), BF),
        V((8, 128, 8), F32),
        V((2, 128, 128), F32),
        V((8, 64, 128), F32), V((8, 64, 128), F32),
        V((2, 8, 128, 128), F32),
        V((2, 8, 128), F32), V((8, 8, 128), F32), V((8, 128), F32), V((4, 8, 128), F32),
        V((4, 32, 128), F32), V((4, 32, 128), F32), V((4, 32, 128), F32), V((4, 32, 128), F32),
        V((64, 2048), F32), V((128, 256), F32), V((1, 128), F32),
        D((8,)), D((7,)), D((8,)), D((3,)), D((4,)), D((3,)), D((4,)), D((7,)), D((8,)), D((7,)), D((8,)),
        D((7,)), D((8,)), D((7,)), D((8,)), D(()), D(()), D((7,)), D((8,)), D((3,)), D((4,)),
        D((3,)), D((4,)), D((3,)), D((4,)), D((3,)),
    ]
    xva, coef_sens, feature_sens = pl.pallas_call(
        kernel,
        out_shape=(
            jax.ShapeDtypeStruct((1, 128), F32),
            jax.ShapeDtypeStruct((64, 2048), F32),
            jax.ShapeDtypeStruct((128, 256), F32),
        ),
        in_specs=[anywhere] + [vmem] * 7,
        out_specs=(anywhere, anywhere, anywhere),
        scratch_shapes=scratch,
        compiler_params=pltpu.CompilerParams(collective_id=0, has_side_effects=True, vmem_limit_bytes=48 << 20),
    )(
        coefficients, factors, feat_factor.reshape(1, -1), feat_degree.reshape(1, -1),
        set_of_trade.reshape(1, -1), party_of_set.reshape(1, -1), threshold.reshape(1, -1), weight.reshape(1, -1),
    )
    return xva.reshape(-1), coef_sens, feature_sens


def solution(mesh):
    placed = (P("scen", None), P(), P(), P(None, "trade"), P("trade"), P("trade"), P(), P())
    return jax.shard_map(
        local,
        mesh=mesh,
        in_specs=placed,
        out_specs=(P("trade"), P("scen", "trade"), P("trade", "scen")),
        check_vma=False,
    )
```

```python
import jax
import jax.numpy as jnp
from jax import lax
from jax.experimental import pallas as pl
from jax.experimental.pallas import tpu as pltpu
from jax.sharding import PartitionSpec as P

MAXDEG = 12
SCEN = 4096
MESH = pl.DeviceIdType.MESH
BF = jnp.bfloat16
F32 = jnp.float32


def mm(left, right):
    return lax.dot_general(left, right, (((1,), (0,)), ((), ())), preferred_element_type=F32)


def mm_nt(left, right):
    return lax.dot_general(left, right, (((1,), (1,)), ((), ())), preferred_element_type=F32)


def halves(value):
    high = value.astype(BF)
    return high, (value - high.astype(F32)).astype(BF)


def thirds(value):
    high = value.astype(BF)
    rest = value - high.astype(F32)
    mid = rest.astype(BF)
    return high, mid, (rest - mid.astype(F32)).astype(BF)


def iota(shape, dim):
    return lax.broadcasted_iota(jnp.int32, shape, dim)


def onehot(mask):
    return jnp.where(mask, 1.0, 0.0).astype(BF)


def upright(row):
    return jnp.broadcast_to(row, (128, 128)).T


def degree_basis(dup, out_h, out_l):
    low = iota((64, 128), 1) < 64
    for r in range(4):
        rows = slice(64 * r, 64 * r + 64)
        current = dup[rows, :]
        twice = current + current
        before = jnp.ones_like(current)
        for pair in range(MAXDEG // 2):
            after = twice * current - before
            cols = slice(128 * pair, 128 * pair + 128)
            out_h[rows, cols], out_l[rows, cols] = halves(jnp.where(low, current, after))
            if pair < MAXDEG // 2 - 1:
                before, current = after, twice * after - current


def kernel(
    coef_hbm, fac_hbm, ff_hbm, fd_hbm, sot_hbm, pos_hbm, thr_hbm, w_hbm,
    xva_out, coef_out, feat_out,
    ff_ref, fd_ref, sot_ref, pos_ref, thr_ref, w_ref, cbuf,
    member, memt, pick, dup, th, tl, fax, faz, pha_h, pha_l, phb_h, phb_l,
    folded, gsum, frows, etb, eh, ehl, party, pcol, same, ownp, tw, sas, sa, sb, sat,
    xs, xr, xt, xz, ga, gb, gra, grb, i_sem,
    c_sem, p_snd, p_rcv, fx_snd, fx_rcv, fz_snd, fz_rcv, e_snd, e_rcv, f_snd, f_rcv,
    sa_snd, sa_rcv, sb_snd, sb_rcv, st_snd, st_rcv, x_snd, x_rcv, x2_snd, x2_rcv,
    ga_snd, ga_rcv, gb_snd, gb_rcv,
):
    t = lax.axis_index("trade")
    sigma = lax.axis_index("scen")
    y, c = t // 2, t % 2
    z, x = sigma // 4, sigma % 4
    partner = 2 * y + 1 - c

    def remote(src, dst, snd, rcv, trade, scen):
        return pltpu.make_async_remote_copy(
            src_ref=src, dst_ref=dst, send_sem=snd, recv_sem=rcv,
            device_id=(trade, scen), device_id_type=MESH,
        )

    def tr(k):
        return lax.rem(t + k, 8)

    def xpeer(k):
        return z * 4 + lax.rem(x + k, 4)

    def zpeer(k):
        return lax.rem(z + k, 4) * 4 + x

    class Gather:
        def __init__(self, slots, snd, rcv, mine, place):
            self.slots, self.snd, self.rcv, self.mine, self.place = slots, snd, rcv, mine, place
            self.sends = []

        def put(self, src, slot, i, k, d):
            trade, scen = self.place(k, d)
            send = remote(src, self.slots.at[slot], self.snd.at[i], self.rcv.at[slot], trade, scen)
            send.start()
            self.sends.append(send)

        def start(self, piece):
            slot = 2 * self.mine + c
            self.put(piece(c), slot, 0, 1, c)
            self.put(piece(1 - c), slot, 1, 3, 1 - c)
            self.put(piece(1 - c), slot, 2, 1, 1 - c)
            self.put(piece(c), slot, 3, 3, c)
            self.put(piece(1 - c), slot, 4, 0, 1 - c)

        def wait_slot(self, k, e):
            slot = 2 * lax.rem(self.mine + k, 4) + lax.rem(c + e, 2)
            trade, scen = self.place(k, lax.rem(c + e, 2)) if k or e else self.place(0, 1 - c)
            remote(self.slots.at[slot], self.slots.at[slot], self.snd.at[0], self.rcv.at[slot], trade, scen).wait_recv()
            return slot

        def forward(self):
            slot = self.wait_slot(3, 0)
            self.put(self.slots.at[slot], slot, 5, 1, c)
            slot = self.wait_slot(1, 1)
            self.put(self.slots.at[slot], slot, 6, 3, c)

        def finish(self):
            for k, e in ((0, 1), (3, 1), (1, 0), (2, 0), (2, 1)):
                self.wait_slot(k, e)

    smalls = []
    for i, (src, dst) in enumerate((
        (sot_hbm, sot_ref), (ff_hbm, ff_ref), (fd_hbm, fd_ref), (fac_hbm, fax.at[x]), (fac_hbm, faz.at[z]),
        (pos_hbm, pos_ref), (thr_hbm, thr_ref), (w_hbm, w_ref),
    )):
        small = pltpu.make_async_copy(src, dst, i_sem.at[i])
        small.start()
        smalls.append(small)
    loads = []
    for i in range(8):
        rows = pl.ds(128 * i, 128)
        load = pltpu.make_async_copy(coef_hbm.at[rows], cbuf.at[rows], c_sem.at[i])
        load.start()
        loads.append(load)

    barrier = pltpu.get_barrier_semaphore()
    for k in range(1, 8):
        pl.semaphore_signal(barrier, inc=1, device_id=(tr(k), sigma), device_id_type=MESH)
    for k in range(1, 4):
        for d in range(2):
            pl.semaphore_signal(barrier, inc=1, device_id=(2 * y + d, xpeer(k)), device_id_type=MESH)
            pl.semaphore_signal(barrier, inc=1, device_id=(2 * y + d, zpeer(k)), device_id_type=MESH)

    for small in smalls:
        small.wait()

    base = (128 * t).astype(F32)
    lanes = iota((128, 128), 1).astype(F32)
    for j in range(16):
        col = upright(sot_ref[:, 128 * j:128 * j + 128].astype(F32) - base)
        member[128 * j:128 * j + 128, :] = onehot(col == lanes)

    def doubled(facts):
        return jnp.concatenate([facts, facts], axis=0).T

    degree_basis(doubled(fax[x]), th, tl)

    keys = (fd_ref[...] - 1) * 64 + ff_ref[...]
    for i in range(4):
        loads[2 * i].wait()
        loads[2 * i + 1].wait()
        rows = slice(256 * i, 256 * i + 256)
        high, low = halves(cbuf[rows, :])
        fold = mm(high, member[...]) + mm(low, member[...])
        folded[2 * i] = fold[:128, :]
        folded[2 * i + 1] = fold[128:, :]
        spot = onehot(iota((768, 256), 0) == keys[:, rows])
        wide = mm(spot, jnp.concatenate(halves(fold), axis=1))
        wide = wide[:, :128] + wide[:, 128:]
        if i == 0:
            gsum[...] = wide
        elif i < 3:
            gsum[...] += wide
        else:
            total = gsum[...] + wide
    high, low = halves(total)
    wide = mm(th[...], jnp.concatenate([high, low], axis=1))
    exposure = wide[:, :128] + wide[:, 128:] + mm(tl[...], high)
    etb[0] = exposure[0:128, :].T
    etb[1] = exposure[128:256, :].T

    pl.semaphore_wait(barrier, 19)

    e_all = Gather(eh, e_snd, e_rcv, y, lambda k, d: (2 * lax.rem(y + k, 4) + d, sigma))
    e_all.start(lambda d: etb.at[d])

    party_sends = []
    for k in range(1, 8):
        send = remote(pos_ref, party.at[t], p_snd.at[k - 1], p_rcv.at[t], tr(k), sigma)
        send.start()
        party_sends.append(send)
    fac_sends = []
    for k in range(1, 4):
        send = remote(fax.at[x], fax.at[x], fx_snd.at[k - 1], fx_rcv.at[x], t, xpeer(k))
        send.start()
        fac_sends.append(send)
        send = remote(faz.at[z], faz.at[z], fz_snd.at[k - 1], fz_rcv.at[z], t, zpeer(k))
        send.start()
        fac_sends.append(send)
    party[t] = pos_ref[...]
    eh[t] = etb[c]
    frows[t] = folded[t]

    fvals = jnp.concatenate([ff_ref[...].astype(F32), fd_ref[...].astype(F32), jnp.zeros((6, 1024), F32)], axis=0).astype(BF)
    lane256 = iota((1024, 256), 1)
    fidx_a = ((lane256 // 64) * 4 + x) * 64 + lane256 % 64
    fidx_b = z * 256 + lane256
    for i, fidx in enumerate((fidx_a, fidx_b)):
        picked = mm(fvals, onehot(iota((1024, 256), 0) == fidx)).astype(jnp.int32)
        pick[i] = onehot(iota((768, 256), 0) == (picked[1:2, :] - 1) * 64 + picked[0:1, :])

    for k in range(1, 8):
        src = tr(k)
        remote(pos_ref, party.at[src], p_snd.at[k - 1], p_rcv.at[src], src, sigma).wait_recv()
    for j in range(8):
        pcol[j] = upright(party[j].astype(F32))
    table = thirds(thr_ref[...]) + thirds(w_ref[...])
    table = jnp.concatenate([part.astype(F32) for part in table] + [jnp.zeros((2, 1024), F32)], axis=0).astype(BF)

    def rows_of(j, carry):
        col = pcol[j]
        rows = pl.ds(pl.multiple_of(j * 128, 128), 128)
        for i in range(8):
            same[rows, 128 * i:128 * i + 128] = onehot(col == party[i].astype(F32))
        spread = jnp.concatenate([onehot(col == lanes + 128.0 * i) for i in range(8)], axis=1)
        tw[j] = mm_nt(spread, table)
        return carry

    lax.fori_loop(0, 8, rows_of, 0)

    e_all.forward()

    def phi_of(buf, which, out_h, out_l):
        def block(q, carry):
            degree_basis(doubled(buf[q]), th, tl)
            out_h[q] = mm(th[...], pick[which]).astype(BF)
            out_l[q] = mm(tl[...], pick[which]).astype(BF)
            return carry

        lax.fori_loop(0, 4, block, 0)

    for k in range(1, 4):
        src = lax.rem(x + k, 4)
        remote(fax.at[x], fax.at[src], fx_snd.at[k - 1], fx_rcv.at[src], t, xpeer(k)).wait_recv()
    phi_of(fax, 0, pha_h, pha_l)

    e_all.finish()
    for j in range(8):
        high, low = halves(eh[j])
        ehl[128 * j:128 * j + 128, 0:128] = high
        ehl[128 * j:128 * j + 128, 128:256] = low

    def adjoint(j, blocks=1):
        rows = pl.ds(pl.multiple_of(j * 128, 128), 128)
        wide = mm(same[rows, :], ehl[...])
        consts = tw[j]
        shift = consts[:, 0:1] + consts[:, 1:2] + consts[:, 2:3]
        scale = consts[:, 3:4] + consts[:, 4:5] + consts[:, 5:6]
        return scale * jax.nn.sigmoid(wide[:, :128] + wide[:, 128:] - shift)

    for d in range(2):
        sas[d] = adjoint(2 * y + d)

    a_all = Gather(sa, sa_snd, sa_rcv, x, lambda k, d: (2 * y + d, xpeer(k)))
    b_all = Gather(sb, sb_snd, sb_rcv, z, lambda k, d: (2 * y + d, zpeer(k)))
    a_all.start(lambda d: sas.at[d, pl.ds(0, 64)])
    b_all.start(lambda d: sas.at[d, pl.ds(64, 64)])
    f_sends = []
    for k in (4, 5, 3, 2, 6, 7, 1):
        other = tr(k)
        send = remote(folded.at[other], frows.at[t], f_snd.at[k - 1], f_rcv.at[t], other, sigma)
        send.start()
        f_sends.append(send)
    sa[2 * x + c] = sas[c, 0:64, :]
    sb[2 * z + c] = sas[c, 64:128, :]
    sat[c, 2 * y] = sas[0]
    sat[c, 2 * y + 1] = sas[1]

    for k in range(2, 8):
        j = lax.rem(2 * y + k, 8)
        sat[c, j] = adjoint(j)
    sat_send = remote(sat.at[c], sat.at[c], st_snd, st_rcv, partner, sigma)
    sat_send.start()

    a_all.forward()
    b_all.forward()

    for k in range(1, 4):
        src = lax.rem(z + k, 4)
        remote(faz.at[z], faz.at[src], fz_snd.at[k - 1], fz_rcv.at[src], t, zpeer(k)).wait_recv()
    phi_of(faz, 1, phb_h, phb_l)

    low_lanes = iota((32, 128), 1) < 64

    def gradient(slots, out_h, out_l, dest):
        total = jnp.zeros((64, 256), F32)
        for q in range(4):
            high, low = halves(jnp.concatenate([slots[2 * q], slots[2 * q + 1]], axis=1))
            total = total + mm(high, out_h[q]) + mm(low, out_h[q]) + mm(high, out_l[q])
        for pair in range(2):
            top = total[0:32, 128 * pair:128 * pair + 128]
            bottom = total[32:64, 128 * pair:128 * pair + 128]
            dest[2 * pair] = jnp.where(low_lanes, top, pltpu.roll(bottom, 64, 1))
            dest[2 * pair + 1] = jnp.where(low_lanes, pltpu.roll(top, 64, 1), bottom)

    g_sends = []
    a_all.finish()
    gradient(sa, pha_h, pha_l, ga)
    for k in (2, 1, 3):
        send = remote(ga.at[lax.rem(z + k, 4)], gra.at[z], ga_snd.at[k - 1], ga_rcv.at[z], t, zpeer(k))
        send.start()
        g_sends.append(send)
    b_all.finish()
    gradient(sb, phb_h, phb_l, gb)
    for k in (2, 1, 3):
        send = remote(gb.at[lax.rem(x + k, 4)], grb.at[x], gb_snd.at[k - 1], gb_rcv.at[x], t, xpeer(k))
        send.start()
        g_sends.append(send)
    gra[z] = ga[z]
    grb[x] = gb[x]

    for i in range(8):
        ownp[:, 128 * i:128 * i + 128] = onehot(iota((256, 128), 0) + 256 * y == party[i])
    wide = mm(ownp[...], ehl[...])
    for d in range(2):
        first = pl.multiple_of(256 * y + 128 * d, 128)
        limit = upright(thr_ref[:, pl.ds(first, 128)])
        soft = jax.nn.softplus(wide[128 * d:128 * d + 128, :128] + wide[128 * d:128 * d + 128, 128:] - limit)
        xs[d] = jnp.broadcast_to(jnp.sum(soft.T, axis=0, keepdims=True), (8, 128))
    x_sends = []
    for k in range(0, 4):
        for e in range(2):
            if k == 0 and e == 0:
                continue
            d = lax.rem(c + e, 2)
            send = remote(xs.at[d], xr.at[2 * x + c], x_snd.at[2 * k + e - 1], x_rcv.at[2 * x + c], 2 * y + d, xpeer(k))
            send.start()
            x_sends.append(send)
    xr[2 * x + c] = xs[c]

    for k in range(1, 8):
        src = tr(k)
        remote(folded.at[0], frows.at[src], f_snd.at[k - 1], f_rcv.at[src], src, sigma).wait_recv()
    remote(sat.at[c], sat.at[1 - c], st_snd, st_rcv, partner, sigma).wait_recv()
    both = jnp.zeros((128, 256), F32)
    for j in range(4):
        left_h, left_l = halves(jnp.concatenate([frows[2 * j], frows[2 * j + 1]], axis=1))
        right = [jnp.concatenate([sat[0, 2 * j + i], sat[1, 2 * j + i]], axis=1) for i in range(2)]
        right_h, right_l = halves(jnp.concatenate(right, axis=0))
        both = both + mm(left_h, right_h) + mm(left_l, right_h) + mm(left_h, right_l)
    feat_out[...] = both

    for k in range(0, 4):
        for e in range(2):
            if k == 0 and e == 0:
                continue
            d = lax.rem(c + e, 2)
            slot = 2 * lax.rem(x + k, 4) + d
            remote(xr.at[slot], xr.at[slot], x_snd.at[2 * k + e - 1], x_rcv.at[slot], 2 * y + d, xpeer(k)).wait_recv()
    part = xr[0]
    for j in range(1, 8):
        part = part + xr[j]
    xt[...] = part
    for k in range(1, 4):
        send = remote(xt, xz.at[z], x2_snd.at[k - 1], x2_rcv.at[z], t, zpeer(k))
        send.start()
        x_sends.append(send)
    xz[z] = part

    row = iota((128, 128), 0)
    of_row = (row // 64) * 32 + ((row % 64) // 32) * 64 + row % 32 + 128 * t
    for j in range(16):
        memt[:, 128 * j:128 * j + 128] = onehot(of_row == sot_ref[:, 128 * j:128 * j + 128])

    for k in range(1, 4):
        src = lax.rem(z + k, 4)
        remote(ga.at[0], gra.at[src], ga_snd.at[k - 1], ga_rcv.at[src], t, zpeer(k)).wait_recv()
    for k in range(1, 4):
        src = lax.rem(x + k, 4)
        remote(gb.at[0], grb.at[src], gb_snd.at[k - 1], gb_rcv.at[src], t, xpeer(k)).wait_recv()
    grad_a = (gra[0] + gra[1]) + (gra[2] + gra[3])
    grad_b = (grb[0] + grb[1]) + (grb[2] + grb[3])
    grads = (jnp.concatenate([grad_a, grad_b], axis=0) * (1.0 / SCEN)).T
    high, low = halves(grads)
    even, odd = memt[0:64, :], memt[64:128, :]
    coef_out[...] = (mm(high[0:64], even) + mm(low[0:64], even)) + (mm(high[64:128], odd) + mm(low[64:128], odd))

    for k in range(1, 4):
        src = lax.rem(z + k, 4)
        remote(xt, xz.at[src], x2_snd.at[k - 1], x2_rcv.at[src], t, zpeer(k)).wait_recv()
    whole = (xz[0] + xz[1]) + (xz[2] + xz[3])
    first = pl.multiple_of(128 * t, 128)
    xva_out[...] = w_ref[:, pl.ds(first, 128)] * whole[0:1, :] * (1.0 / SCEN)

    for send in party_sends + fac_sends + e_all.sends + f_sends + a_all.sends + b_all.sends + [sat_send] + x_sends + g_sends:
        send.wait_send()


def place_outputs(xva, coef, feat, xva_out, coef_out, feat_out, sem):
    copies = []
    for i, (src, dst) in enumerate(((coef, coef_out), (feat, feat_out), (xva, xva_out))):
        copy = pltpu.make_async_copy(src, dst, sem.at[i])
        copy.start()
        copies.append(copy)
    for copy in copies:
        copy.wait()


def local(factors, feat_factor, feat_degree, coefficients, set_of_trade, party_of_set, threshold, weight):
    vmem = pl.BlockSpec(memory_space=pltpu.VMEM)
    hbm = pl.BlockSpec(memory_space=pltpu.HBM)
    V = pltpu.VMEM
    D = pltpu.SemaphoreType.DMA
    scratch = [
        V((1, 1024), jnp.int32), V((1, 1024), jnp.int32), V((1, 2048), jnp.int32),
        V((1, 128), jnp.int32), V((1, 1024), F32), V((1, 1024), F32),
        V((1024, 2048), F32),
        V((2048, 128), BF),
        V((128, 2048), BF),
        V((2, 768, 256), BF),
        V((256, 128), F32),
        V((256, 768), BF), V((256, 768), BF),
        V((4, 64, 256), F32), V((4, 64, 256), F32),
        V((4, 256, 256), BF), V((4, 256, 256), BF), V((4, 256, 256), BF), V((4, 256, 256), BF),
        V((8, 128, 128), F32),
        V((768, 128), F32),
        V((8, 128, 128), F32),
        V((2, 128, 128), F32),
        V((8, 128, 128), F32),
        V((1024, 256), BF),
        V((8, 1, 128), jnp.int32),
        V((8, 128, 128), F32),
        V((1024, 1024), BF),
        V((256, 1024), BF),
        V((8, 128, 8), F32),
        V((2, 128, 128), F32),
        V((8, 64, 128), F32), V((8, 64, 128), F32),
        V((2, 8, 128, 128), F32),
        V((2, 8, 128), F32), V((8, 8, 128), F32), V((8, 128), F32), V((4, 8, 128), F32),
        V((4, 32, 128), F32), V((4, 32, 128), F32), V((4, 32, 128), F32), V((4, 32, 128), F32),
        D((8,)), D((8,)), D((7,)), D((8,)), D((3,)), D((4,)), D((3,)), D((4,)), D((7,)), D((8,)), D((7,)), D((8,)),
        D((7,)), D((8,)), D((7,)), D((8,)), D(()), D(()), D((7,)), D((8,)), D((3,)), D((4,)),
        D((3,)), D((4,)), D((3,)), D((4,)),
    ]
    shapes = (
        jax.ShapeDtypeStruct((1, 128), F32),
        jax.ShapeDtypeStruct((64, 2048), F32),
        jax.ShapeDtypeStruct((128, 256), F32),
    )
    results = pl.pallas_call(
        kernel,
        out_shape=shapes,
        in_specs=[hbm] * 8,
        out_specs=(vmem, vmem, vmem),
        scratch_shapes=scratch,
        compiler_params=pltpu.CompilerParams(collective_id=0, has_side_effects=True, vmem_limit_bytes=40 << 20),
    )(*[
        pltpu.with_memory_space_constraint(array, pltpu.HBM)
        for array in (
            coefficients, factors.T, feat_factor.reshape(1, -1), feat_degree.reshape(1, -1),
            set_of_trade.reshape(1, -1), party_of_set.reshape(1, -1), threshold.reshape(1, -1), weight.reshape(1, -1),
        )
    ])
    xva, coef_sens, feature_sens = pl.pallas_call(
        place_outputs,
        out_shape=shapes,
        in_specs=[vmem] * 3,
        out_specs=(hbm, hbm, hbm),
        scratch_shapes=[D((3,))],
        compiler_params=pltpu.CompilerParams(vmem_limit_bytes=4 << 20),
    )(*results)
    return xva.reshape(-1), coef_sens, feature_sens


def solution(mesh):
    placed = (P("scen", None), P(), P(), P(None, "trade"), P("trade"), P("trade"), P(), P())
    return jax.shard_map(
        local,
        mesh=mesh,
        in_specs=placed,
        out_specs=(P("trade"), P("scen", "trade"), P("trade", "scen")),
        check_vma=False,
    )
```

```python
import jax
import jax.numpy as jnp
from jax import lax
from jax.experimental import pallas as pl
from jax.experimental.pallas import tpu as pltpu
from jax.sharding import PartitionSpec as P

MAXDEG = 12
SCEN = 4096
MESH = pl.DeviceIdType.MESH
BF = jnp.bfloat16
F32 = jnp.float32


def mm(left, right):
    return lax.dot_general(left, right, (((1,), (0,)), ((), ())), preferred_element_type=F32)


def mm_nt(left, right):
    return lax.dot_general(left, right, (((1,), (1,)), ((), ())), preferred_element_type=F32)


def halves(value):
    high = value.astype(BF)
    return high, (value - high.astype(F32)).astype(BF)


def thirds(value):
    high = value.astype(BF)
    rest = value - high.astype(F32)
    mid = rest.astype(BF)
    return high, mid, (rest - mid.astype(F32)).astype(BF)


def iota(shape, dim):
    return lax.broadcasted_iota(jnp.int32, shape, dim)


def onehot(mask):
    return jnp.where(mask, 1.0, 0.0).astype(BF)


def upright(row):
    return jnp.broadcast_to(row, (128, 128)).T


def degree_basis(dup, out_h, out_l):
    low = iota((64, 128), 1) < 64
    for r in range(4):
        rows = slice(64 * r, 64 * r + 64)
        current = dup[rows, :]
        twice = current + current
        before = jnp.ones_like(current)
        for pair in range(MAXDEG // 2):
            after = twice * current - before
            cols = slice(128 * pair, 128 * pair + 128)
            out_h[rows, cols], out_l[rows, cols] = halves(jnp.where(low, current, after))
            if pair < MAXDEG // 2 - 1:
                before, current = after, twice * after - current


def kernel(
    coef_hbm, fac_hbm, ff_hbm, fd_hbm, sot_hbm, pos_hbm, thr_hbm, w_hbm,
    xva_out, coef_out, feat_out,
    ff_ref, fd_ref, sot_ref, pos_ref, thr_ref, w_ref, cbuf,
    member, memt, pick, th, tl, fax, faz, pha_h, pha_l, phb_h, phb_l,
    spot, fparts, folded, gsum, frows, etb, eh, ehl, party, pcol, same, ownp, tw, sas, sa, sb, sat,
    xs, xr, xt, xz, ga, gb, gra, grb, i_sem,
    c_sem, p_snd, p_rcv, fx_snd, fx_rcv, fz_snd, fz_rcv, e_snd, e_rcv, f_snd, f_rcv,
    sa_snd, sa_rcv, sb_snd, sb_rcv, st_snd, st_rcv, x_snd, x_rcv, x2_snd, x2_rcv,
    ga_snd, ga_rcv, gb_snd, gb_rcv,
):
    t = lax.axis_index("trade")
    sigma = lax.axis_index("scen")
    y, c = t // 2, t % 2
    z, x = sigma // 4, sigma % 4
    partner = 2 * y + 1 - c

    def remote(src, dst, snd, rcv, trade, scen):
        return pltpu.make_async_remote_copy(
            src_ref=src, dst_ref=dst, send_sem=snd, recv_sem=rcv,
            device_id=(trade, scen), device_id_type=MESH,
        )

    def tr(k):
        return lax.rem(t + k, 8)

    def xpeer(k):
        return z * 4 + lax.rem(x + k, 4)

    def zpeer(k):
        return lax.rem(z + k, 4) * 4 + x

    class Gather:
        def __init__(self, slots, snd, rcv, mine, place):
            self.slots, self.snd, self.rcv, self.mine, self.place = slots, snd, rcv, mine, place
            self.sends = []

        def put(self, src, slot, i, k, d):
            trade, scen = self.place(k, d)
            send = remote(src, self.slots.at[slot], self.snd.at[i], self.rcv.at[slot], trade, scen)
            send.start()
            self.sends.append(send)

        def start(self, piece):
            slot = 2 * self.mine + c
            self.put(piece(c), slot, 0, 1, c)
            self.put(piece(1 - c), slot, 1, 3, 1 - c)
            self.put(piece(1 - c), slot, 2, 1, 1 - c)
            self.put(piece(c), slot, 3, 3, c)
            self.put(piece(1 - c), slot, 4, 0, 1 - c)

        def start_direct(self, piece):
            slot = 2 * self.mine + c
            for i, (k, e) in enumerate(((2, 0), (2, 1), (1, 0), (3, 0), (1, 1), (3, 1), (0, 1))):
                d = lax.rem(c + e, 2)
                self.put(piece(d), slot, i, k, d)

        def finish_direct(self):
            for k, e in ((0, 1), (3, 0), (3, 1), (1, 0), (1, 1), (2, 0), (2, 1)):
                self.wait_slot(k, e)

        def wait_slot(self, k, e):
            slot = 2 * lax.rem(self.mine + k, 4) + lax.rem(c + e, 2)
            trade, scen = self.place(k, lax.rem(c + e, 2)) if k or e else self.place(0, 1 - c)
            remote(self.slots.at[slot], self.slots.at[slot], self.snd.at[0], self.rcv.at[slot], trade, scen).wait_recv()
            return slot

        def forward(self):
            slot = self.wait_slot(3, 0)
            self.put(self.slots.at[slot], slot, 5, 1, c)
            slot = self.wait_slot(1, 1)
            self.put(self.slots.at[slot], slot, 6, 3, c)

        def finish(self):
            for k, e in ((0, 1), (3, 1), (1, 0), (2, 0), (2, 1)):
                self.wait_slot(k, e)

    smalls = []
    for i, (src, dst) in enumerate((
        (sot_hbm, sot_ref), (ff_hbm, ff_ref), (fd_hbm, fd_ref), (fac_hbm, fax.at[x]), (fac_hbm, faz.at[z]),
        (pos_hbm, pos_ref), (thr_hbm, thr_ref), (w_hbm, w_ref),
    )):
        small = pltpu.make_async_copy(src, dst, i_sem.at[i])
        small.start()
        smalls.append(small)
    loads = []
    for i in range(8):
        rows = pl.ds(128 * i, 128)
        loads.append(pltpu.make_async_copy(coef_hbm.at[rows], cbuf.at[rows], c_sem.at[i]))
    for load in loads[:2]:
        load.start()
    barrier = pltpu.get_barrier_semaphore()
    for k in range(1, 8):
        pl.semaphore_signal(barrier, inc=1, device_id=(tr(k), sigma), device_id_type=MESH)
    for k in range(1, 4):
        for d in range(2):
            pl.semaphore_signal(barrier, inc=1, device_id=(2 * y + d, xpeer(k)), device_id_type=MESH)
            pl.semaphore_signal(barrier, inc=1, device_id=(2 * y + d, zpeer(k)), device_id_type=MESH)

    for small in smalls:
        small.wait()
    for load in loads[2:]:
        load.start()

    base = (128 * t).astype(F32)
    lanes = iota((128, 128), 1).astype(F32)
    for j in range(16):
        col = upright(sot_ref[:, 128 * j:128 * j + 128].astype(F32) - base)
        member[128 * j:128 * j + 128, :] = onehot(col == lanes)

    def doubled(facts):
        return jnp.concatenate([facts, facts], axis=0).T

    degree_basis(doubled(fax[x]), th, tl)

    keys = (fd_ref[...] - 1) * 64 + ff_ref[...]
    for i in range(8):
        cols = slice(128 * i, 128 * i + 128)
        spot[:, cols] = onehot(iota((768, 128), 0) == keys[:, cols])

    def regroup(i):
        rows = slice(256 * i, 256 * i + 256)
        wide = mm(spot[:, rows], fparts[rows, :])
        return wide[:, :128] + wide[:, 128:]

    for i in range(4):
        loads[2 * i].wait()
        loads[2 * i + 1].wait()
        rows = slice(256 * i, 256 * i + 256)
        high, low = halves(cbuf[rows, :])
        fold = mm(high, member[...]) + mm(low, member[...])
        folded[2 * i] = fold[:128, :]
        folded[2 * i + 1] = fold[128:, :]
        high, low = halves(fold)
        fparts[rows, 0:128] = high
        fparts[rows, 128:256] = low
        if i == 1:
            gsum[...] = regroup(0)
        elif i > 1:
            gsum[...] += regroup(i - 1)
        if i == 1:
            pl.semaphore_wait(barrier, 19)
            party_sends = []
            for k in range(1, 8):
                send = remote(pos_ref, party.at[t], p_snd.at[k - 1], p_rcv.at[t], tr(k), sigma)
                send.start()
                party_sends.append(send)
            fac_sends = []
            for k in range(1, 4):
                send = remote(fax.at[x], fax.at[x], fx_snd.at[k - 1], fx_rcv.at[x], t, xpeer(k))
                send.start()
                fac_sends.append(send)
                send = remote(faz.at[z], faz.at[z], fz_snd.at[k - 1], fz_rcv.at[z], t, zpeer(k))
                send.start()
                fac_sends.append(send)
            party[t] = pos_ref[...]
    high, low = halves(gsum[...] + regroup(3))
    wide = mm(th[...], jnp.concatenate([high, low], axis=1))
    exposure = wide[:, :128] + wide[:, 128:] + mm(tl[...], high)
    etb[0] = exposure[0:128, :].T
    etb[1] = exposure[128:256, :].T

    e_all = Gather(eh, e_snd, e_rcv, y, lambda k, d: (2 * lax.rem(y + k, 4) + d, sigma))
    e_all.start(lambda d: etb.at[d])

    eh[t] = etb[c]
    frows[t] = folded[t]

    fvals = jnp.concatenate([ff_ref[...].astype(F32), fd_ref[...].astype(F32), jnp.zeros((6, 1024), F32)], axis=0).astype(BF)
    lane256 = iota((1024, 256), 1)
    fidx_a = ((lane256 // 64) * 4 + x) * 64 + lane256 % 64
    fidx_b = z * 256 + lane256
    for i, fidx in enumerate((fidx_a, fidx_b)):
        picked = mm(fvals, onehot(iota((1024, 256), 0) == fidx)).astype(jnp.int32)
        pick[i] = onehot(iota((768, 256), 0) == (picked[1:2, :] - 1) * 64 + picked[0:1, :])

    for k in range(1, 8):
        src = tr(k)
        remote(pos_ref, party.at[src], p_snd.at[k - 1], p_rcv.at[src], src, sigma).wait_recv()
    for j in range(8):
        pcol[j] = upright(party[j].astype(F32))
    table = thirds(thr_ref[...]) + thirds(w_ref[...])
    table = jnp.concatenate([part.astype(F32) for part in table] + [jnp.zeros((2, 1024), F32)], axis=0).astype(BF)

    def rows_of(j, carry):
        col = pcol[j]
        rows = pl.ds(pl.multiple_of(j * 128, 128), 128)
        for i in range(8):
            same[rows, 128 * i:128 * i + 128] = onehot(col == party[i].astype(F32))
        spread = jnp.concatenate([onehot(col == lanes + 128.0 * i) for i in range(8)], axis=1)
        tw[j] = mm_nt(spread, table)
        return carry

    lax.fori_loop(0, 8, rows_of, 0)

    e_all.forward()

    def phi_of(buf, which, out_h, out_l):
        def block(q, carry):
            degree_basis(doubled(buf[q]), th, tl)
            out_h[q] = mm(th[...], pick[which]).astype(BF)
            out_l[q] = mm(tl[...], pick[which]).astype(BF)
            return carry

        lax.fori_loop(0, 4, block, 0)

    for k in range(1, 4):
        src = lax.rem(x + k, 4)
        remote(fax.at[x], fax.at[src], fx_snd.at[k - 1], fx_rcv.at[src], t, xpeer(k)).wait_recv()
    phi_of(fax, 0, pha_h, pha_l)

    e_all.finish()
    for j in range(8):
        high, low = halves(eh[j])
        ehl[128 * j:128 * j + 128, 0:128] = high
        ehl[128 * j:128 * j + 128, 128:256] = low

    def adjoint(j, blocks=1):
        rows = pl.ds(pl.multiple_of(j * 128, 128), 128)
        wide = mm(same[rows, :], ehl[...])
        consts = tw[j]
        shift = consts[:, 0:1] + consts[:, 1:2] + consts[:, 2:3]
        scale = consts[:, 3:4] + consts[:, 4:5] + consts[:, 5:6]
        return scale * jax.nn.sigmoid(wide[:, :128] + wide[:, 128:] - shift)

    for d in range(2):
        sas[d] = adjoint(2 * y + d)

    a_all = Gather(sa, sa_snd, sa_rcv, x, lambda k, d: (2 * y + d, xpeer(k)))
    b_all = Gather(sb, sb_snd, sb_rcv, z, lambda k, d: (2 * y + d, zpeer(k)))
    a_all.start_direct(lambda d: sas.at[d, pl.ds(0, 64)])
    b_all.start_direct(lambda d: sas.at[d, pl.ds(64, 64)])
    f_sends = []
    for k in (4, 5, 3, 2, 6, 7, 1):
        other = tr(k)
        send = remote(folded.at[other], frows.at[t], f_snd.at[k - 1], f_rcv.at[t], other, sigma)
        send.start()
        f_sends.append(send)
    sa[2 * x + c] = sas[c, 0:64, :]
    sb[2 * z + c] = sas[c, 64:128, :]
    sat[c, 2 * y] = sas[0]
    sat[c, 2 * y + 1] = sas[1]

    for k in range(2, 8):
        j = lax.rem(2 * y + k, 8)
        sat[c, j] = adjoint(j)
    sat_send = remote(sat.at[c], sat.at[c], st_snd, st_rcv, partner, sigma)
    sat_send.start()

    for i in range(8):
        ownp[:, 128 * i:128 * i + 128] = onehot(iota((256, 128), 0) + 256 * y == party[i])
    wide = mm(ownp[...], ehl[...])
    for d in range(2):
        first = pl.multiple_of(256 * y + 128 * d, 128)
        limit = upright(thr_ref[:, pl.ds(first, 128)])
        soft = jax.nn.softplus(wide[128 * d:128 * d + 128, :128] + wide[128 * d:128 * d + 128, 128:] - limit)
        xs[d] = jnp.broadcast_to(jnp.sum(soft.T, axis=0, keepdims=True), (8, 128))
    x_sends = []
    for k in range(0, 4):
        for e in range(2):
            if k == 0 and e == 0:
                continue
            d = lax.rem(c + e, 2)
            send = remote(xs.at[d], xr.at[2 * x + c], x_snd.at[2 * k + e - 1], x_rcv.at[2 * x + c], 2 * y + d, xpeer(k))
            send.start()
            x_sends.append(send)
    xr[2 * x + c] = xs[c]

    for k in range(1, 4):
        src = lax.rem(z + k, 4)
        remote(faz.at[z], faz.at[src], fz_snd.at[k - 1], fz_rcv.at[src], t, zpeer(k)).wait_recv()
    phi_of(faz, 1, phb_h, phb_l)

    low_lanes = iota((32, 128), 1) < 64

    def gradient(slots, out_h, out_l, dest):
        total = jnp.zeros((64, 256), F32)
        for q in range(4):
            high, low = halves(jnp.concatenate([slots[2 * q], slots[2 * q + 1]], axis=1))
            total = total + mm(high, out_h[q]) + mm(low, out_h[q]) + mm(high, out_l[q])
        for pair in range(2):
            top = total[0:32, 128 * pair:128 * pair + 128]
            bottom = total[32:64, 128 * pair:128 * pair + 128]
            dest[2 * pair] = jnp.where(low_lanes, top, pltpu.roll(bottom, 64, 1))
            dest[2 * pair + 1] = jnp.where(low_lanes, pltpu.roll(top, 64, 1), bottom)

    g_sends = []
    a_all.finish_direct()
    gradient(sa, pha_h, pha_l, ga)
    for k in (2, 1, 3):
        send = remote(ga.at[lax.rem(z + k, 4)], gra.at[z], ga_snd.at[k - 1], ga_rcv.at[z], t, zpeer(k))
        send.start()
        g_sends.append(send)
    b_all.finish_direct()
    gradient(sb, phb_h, phb_l, gb)
    for k in (2, 1, 3):
        send = remote(gb.at[lax.rem(x + k, 4)], grb.at[x], gb_snd.at[k - 1], gb_rcv.at[x], t, xpeer(k))
        send.start()
        g_sends.append(send)
    gra[z] = ga[z]
    grb[x] = gb[x]

    for k in range(0, 4):
        for e in range(2):
            if k == 0 and e == 0:
                continue
            d = lax.rem(c + e, 2)
            slot = 2 * lax.rem(x + k, 4) + d
            remote(xr.at[slot], xr.at[slot], x_snd.at[2 * k + e - 1], x_rcv.at[slot], 2 * y + d, xpeer(k)).wait_recv()
    part = xr[0]
    for j in range(1, 8):
        part = part + xr[j]
    xt[...] = part
    for k in range(1, 4):
        send = remote(xt, xz.at[z], x2_snd.at[k - 1], x2_rcv.at[z], t, zpeer(k))
        send.start()
        x_sends.append(send)
    xz[z] = part

    for k in range(1, 8):
        src = tr(k)
        remote(folded.at[0], frows.at[src], f_snd.at[k - 1], f_rcv.at[src], src, sigma).wait_recv()
    remote(sat.at[c], sat.at[1 - c], st_snd, st_rcv, partner, sigma).wait_recv()
    both = jnp.zeros((128, 256), F32)
    for j in range(4):
        left_h, left_l = halves(jnp.concatenate([frows[2 * j], frows[2 * j + 1]], axis=1))
        right = [jnp.concatenate([sat[0, 2 * j + i], sat[1, 2 * j + i]], axis=1) for i in range(2)]
        right_h, right_l = halves(jnp.concatenate(right, axis=0))
        both = both + mm(left_h, right_h) + mm(left_l, right_h) + mm(left_h, right_l)
    feat_out[...] = both

    row = iota((128, 128), 0)
    of_row = (row // 64) * 32 + ((row % 64) // 32) * 64 + row % 32 + 128 * t
    for j in range(16):
        memt[:, 128 * j:128 * j + 128] = onehot(of_row == sot_ref[:, 128 * j:128 * j + 128])

    for k in range(1, 4):
        src = lax.rem(z + k, 4)
        remote(ga.at[0], gra.at[src], ga_snd.at[k - 1], ga_rcv.at[src], t, zpeer(k)).wait_recv()
    for k in range(1, 4):
        src = lax.rem(x + k, 4)
        remote(gb.at[0], grb.at[src], gb_snd.at[k - 1], gb_rcv.at[src], t, xpeer(k)).wait_recv()
    grad_a = (gra[0] + gra[1]) + (gra[2] + gra[3])
    grad_b = (grb[0] + grb[1]) + (grb[2] + grb[3])
    grads = (jnp.concatenate([grad_a, grad_b], axis=0) * (1.0 / SCEN)).T
    high, low = halves(grads)
    even, odd = memt[0:64, :], memt[64:128, :]
    coef_out[...] = (mm(high[0:64], even) + mm(low[0:64], even)) + (mm(high[64:128], odd) + mm(low[64:128], odd))

    for k in range(1, 4):
        src = lax.rem(z + k, 4)
        remote(xt, xz.at[src], x2_snd.at[k - 1], x2_rcv.at[src], t, zpeer(k)).wait_recv()
    whole = (xz[0] + xz[1]) + (xz[2] + xz[3])
    first = pl.multiple_of(128 * t, 128)
    xva_out[...] = w_ref[:, pl.ds(first, 128)] * whole[0:1, :] * (1.0 / SCEN)

    for send in party_sends + fac_sends + e_all.sends + f_sends + a_all.sends + b_all.sends + [sat_send] + x_sends + g_sends:
        send.wait_send()


def place_outputs(xva, coef, feat, xva_out, coef_out, feat_out, sem):
    copies = []
    for i, (src, dst) in enumerate(((coef, coef_out), (feat, feat_out), (xva, xva_out))):
        copy = pltpu.make_async_copy(src, dst, sem.at[i])
        copy.start()
        copies.append(copy)
    for copy in copies:
        copy.wait()


def local(factors, feat_factor, feat_degree, coefficients, set_of_trade, party_of_set, threshold, weight):
    vmem = pl.BlockSpec(memory_space=pltpu.VMEM)
    hbm = pl.BlockSpec(memory_space=pltpu.HBM)
    V = pltpu.VMEM
    D = pltpu.SemaphoreType.DMA
    scratch = [
        V((1, 1024), jnp.int32), V((1, 1024), jnp.int32), V((1, 2048), jnp.int32),
        V((1, 128), jnp.int32), V((1, 1024), F32), V((1, 1024), F32),
        V((1024, 2048), F32),
        V((2048, 128), BF),
        V((128, 2048), BF),
        V((2, 768, 256), BF),
        V((256, 768), BF), V((256, 768), BF),
        V((4, 64, 256), F32), V((4, 64, 256), F32),
        V((4, 256, 256), BF), V((4, 256, 256), BF), V((4, 256, 256), BF), V((4, 256, 256), BF),
        V((768, 1024), BF),
        V((1024, 256), BF),
        V((8, 128, 128), F32),
        V((768, 128), F32),
        V((8, 128, 128), F32),
        V((2, 128, 128), F32),
        V((8, 128, 128), F32),
        V((1024, 256), BF),
        V((8, 1, 128), jnp.int32),
        V((8, 128, 128), F32),
        V((1024, 1024), BF),
        V((256, 1024), BF),
        V((8, 128, 8), F32),
        V((2, 128, 128), F32),
        V((8, 64, 128), F32), V((8, 64, 128), F32),
        V((2, 8, 128, 128), F32),
        V((2, 8, 128), F32), V((8, 8, 128), F32), V((8, 128), F32), V((4, 8, 128), F32),
        V((4, 32, 128), F32), V((4, 32, 128), F32), V((4, 32, 128), F32), V((4, 32, 128), F32),
        D((8,)), D((8,)), D((7,)), D((8,)), D((3,)), D((4,)), D((3,)), D((4,)), D((7,)), D((8,)), D((7,)), D((8,)),
        D((7,)), D((8,)), D((7,)), D((8,)), D(()), D(()), D((7,)), D((8,)), D((3,)), D((4,)),
        D((3,)), D((4,)), D((3,)), D((4,)),
    ]
    shapes = (
        jax.ShapeDtypeStruct((1, 128), F32),
        jax.ShapeDtypeStruct((64, 2048), F32),
        jax.ShapeDtypeStruct((128, 256), F32),
    )
    results = pl.pallas_call(
        kernel,
        out_shape=shapes,
        in_specs=[hbm] * 8,
        out_specs=(vmem, vmem, vmem),
        scratch_shapes=scratch,
        compiler_params=pltpu.CompilerParams(collective_id=0, has_side_effects=True, vmem_limit_bytes=40 << 20),
    )(*[
        pltpu.with_memory_space_constraint(array, pltpu.HBM)
        for array in (
            coefficients, factors.T, feat_factor.reshape(1, -1), feat_degree.reshape(1, -1),
            set_of_trade.reshape(1, -1), party_of_set.reshape(1, -1), threshold.reshape(1, -1), weight.reshape(1, -1),
        )
    ])
    xva, coef_sens, feature_sens = pl.pallas_call(
        place_outputs,
        out_shape=shapes,
        in_specs=[vmem] * 3,
        out_specs=(hbm, hbm, hbm),
        scratch_shapes=[D((3,))],
        compiler_params=pltpu.CompilerParams(vmem_limit_bytes=4 << 20),
    )(*results)
    return xva.reshape(-1), coef_sens, feature_sens


def solution(mesh):
    placed = (P("scen", None), P(), P(), P(None, "trade"), P("trade"), P("trade"), P(), P())
    return jax.shard_map(
        local,
        mesh=mesh,
        in_specs=placed,
        out_specs=(P("trade"), P("scen", "trade"), P("trade", "scen")),
        check_vma=False,
    )
```

```python
import jax
import jax.numpy as jnp
from jax import lax
from jax.experimental import pallas as pl
from jax.experimental.pallas import tpu as pltpu
from jax.sharding import PartitionSpec as P

MAXDEG = 12
SCEN = 4096
MESH = pl.DeviceIdType.MESH
BF = jnp.bfloat16
F32 = jnp.float32


def mm(left, right):
    return lax.dot_general(left, right, (((1,), (0,)), ((), ())), preferred_element_type=F32)


def mm_nt(left, right):
    return lax.dot_general(left, right, (((1,), (1,)), ((), ())), preferred_element_type=F32)


def halves(value):
    high = value.astype(BF)
    return high, (value - high.astype(F32)).astype(BF)


def thirds(value):
    high = value.astype(BF)
    rest = value - high.astype(F32)
    mid = rest.astype(BF)
    return high, mid, (rest - mid.astype(F32)).astype(BF)


def iota(shape, dim):
    return lax.broadcasted_iota(jnp.int32, shape, dim)


def onehot(mask):
    return jnp.where(mask, 1.0, 0.0).astype(BF)


def upright(row):
    return jnp.broadcast_to(row, (128, 128)).T


def degree_basis(dup, out_h, out_l):
    low = iota((64, 128), 1) < 64
    for r in range(4):
        rows = slice(64 * r, 64 * r + 64)
        current = dup[rows, :]
        twice = current + current
        before = jnp.ones_like(current)
        for pair in range(MAXDEG // 2):
            after = twice * current - before
            cols = slice(128 * pair, 128 * pair + 128)
            out_h[rows, cols], out_l[rows, cols] = halves(jnp.where(low, current, after))
            if pair < MAXDEG // 2 - 1:
                before, current = after, twice * after - current


def kernel(
    coef_hbm, fac_hbm, ff_hbm, fd_hbm, sot_hbm, pos_hbm, thr_hbm, w_hbm,
    xva_out, coef_out, feat_out,
    ff_ref, fd_ref, sot_ref, pos_ref, thr_ref, w_ref, cbuf,
    member, memt, pick, th, tl, fax, faz, pha_h, pha_l, phb_h, phb_l,
    spot, fparts, folded, frows, etb, eh, ehl, party, pcol, same, ownp, tw, sas, sa, sb, sat,
    xs, xr, xt, xz, ga, gb, gra, grb, i_sem,
    c_sem, p_snd, p_rcv, fx_snd, fx_rcv, fz_snd, fz_rcv, e_snd, e_rcv, f_snd, f_rcv,
    sa_snd, sa_rcv, sb_snd, sb_rcv, st_snd, st_rcv, x_snd, x_rcv, x2_snd, x2_rcv,
    ga_snd, ga_rcv, gb_snd, gb_rcv,
):
    t = lax.axis_index("trade")
    sigma = lax.axis_index("scen")
    y, c = t // 2, t % 2
    z, x = sigma // 4, sigma % 4
    partner = 2 * y + 1 - c

    def remote(src, dst, snd, rcv, trade, scen):
        return pltpu.make_async_remote_copy(
            src_ref=src, dst_ref=dst, send_sem=snd, recv_sem=rcv,
            device_id=(trade, scen), device_id_type=MESH,
        )

    def tr(k):
        return lax.rem(t + k, 8)

    def xpeer(k):
        return z * 4 + lax.rem(x + k, 4)

    def zpeer(k):
        return lax.rem(z + k, 4) * 4 + x

    class Gather:
        def __init__(self, slots, snd, rcv, mine, place):
            self.slots, self.snd, self.rcv, self.mine, self.place = slots, snd, rcv, mine, place
            self.sends = []

        def put(self, src, slot, i, k, d):
            trade, scen = self.place(k, d)
            send = remote(src, self.slots.at[slot], self.snd.at[i], self.rcv.at[slot], trade, scen)
            send.start()
            self.sends.append(send)

        def start(self, src, e):
            d = lax.rem(c + e, 2)
            for i, k in enumerate((2, 1, 3) + (() if e == 0 else (0,))):
                self.put(src, 2 * self.mine + c, 4 * e + i, k, d)

        def wait(self, k):
            for e in range(2):
                if k or e:
                    slot = 2 * lax.rem(self.mine + k, 4) + lax.rem(c + e, 2)
                    trade, scen = self.place(k, lax.rem(c + e, 2))
                    here = self.slots.at[slot]
                    remote(here, here, self.snd.at[0], self.rcv.at[slot], trade, scen).wait_recv()

    class Relay(Gather):
        def half(self, slot, h):
            return self.slots.at[slot, pl.ds(64 * h, 64)]

        def put(self, src, slot, i, k, d, h):
            trade, scen = self.place(k, d)
            send = remote(src, self.half(slot, h), self.snd.at[i], self.rcv.at[2 * slot + h], trade, scen)
            send.start()
            self.sends.append(send)

        def start(self, src):
            slot = 2 * self.mine + c
            for i, (k, e) in enumerate(((1, 0), (3, 1), (1, 1), (3, 0), (0, 1))):
                d = lax.rem(c + e, 2)
                for h in range(2):
                    self.put(src.at[d, pl.ds(64 * h, 64)], slot, 2 * i + h, k, d, h)

        def wait(self, k, e, h):
            slot = 2 * lax.rem(self.mine + k, 4) + lax.rem(c + e, 2)
            trade, scen = self.place(k if k else 0, lax.rem(c + e, 2))
            here = self.half(slot, h)
            remote(here, here, self.snd.at[0], self.rcv.at[2 * slot + h], trade, scen).wait_recv()
            return slot

        def forward(self):
            for h in range(2):
                slot = self.wait(3, 0, h)
                self.put(self.half(slot, h), slot, 10 + h, 1, c, h)
                slot = self.wait(1, 1, h)
                self.put(self.half(slot, h), slot, 12 + h, 3, c, h)

        def finish(self):
            for h in range(2):
                for k, e in ((0, 1), (3, 1), (1, 0), (2, 0), (2, 1)):
                    self.wait(k, e, h)

    smalls = []
    for i, (src, dst) in enumerate((
        (sot_hbm, sot_ref), (ff_hbm, ff_ref), (fd_hbm, fd_ref), (fac_hbm, fax.at[x]), (fac_hbm, faz.at[z]),
        (pos_hbm, pos_ref), (thr_hbm, thr_ref), (w_hbm, w_ref),
    )):
        small = pltpu.make_async_copy(src, dst, i_sem.at[i])
        small.start()
        smalls.append(small)
    loads = []
    for i in range(8):
        rows = pl.ds(128 * i, 128)
        loads.append(pltpu.make_async_copy(coef_hbm.at[rows], cbuf.at[rows], c_sem.at[i]))
    for load in loads:
        load.start(priority=1)
    barrier = pltpu.get_barrier_semaphore()
    for k in range(1, 8):
        pl.semaphore_signal(barrier, inc=1, device_id=(tr(k), sigma), device_id_type=MESH)
    for k in range(1, 4):
        for d in range(2):
            pl.semaphore_signal(barrier, inc=1, device_id=(2 * y + d, xpeer(k)), device_id_type=MESH)
            pl.semaphore_signal(barrier, inc=1, device_id=(2 * y + d, zpeer(k)), device_id_type=MESH)

    for small in smalls:
        small.wait()
    base = (128 * t).astype(F32)
    lanes = iota((128, 128), 1).astype(F32)
    for j in range(16):
        col = upright(sot_ref[:, 128 * j:128 * j + 128].astype(F32) - base)
        member[128 * j:128 * j + 128, :] = onehot(col == lanes)

    def doubled(facts):
        return jnp.concatenate([facts, facts], axis=0).T

    degree_basis(doubled(fax[x]), th, tl)

    keys = (fd_ref[...] - 1) * 64 + ff_ref[...]
    for i in range(8):
        cols = slice(128 * i, 128 * i + 128)
        spot[:, cols] = onehot(iota((768, 128), 0) == keys[:, cols])

    def fold_rows(i):
        rows = slice(256 * i, 256 * i + 256)
        high, low = halves(cbuf[rows, :])
        fold = mm(high, member[...]) + mm(low, member[...])
        folded[2 * i] = fold[:128, :]
        folded[2 * i + 1] = fold[128:, :]
        high, low = halves(fold)
        fparts[rows, 0:128] = high
        fparts[rows, 128:256] = low

    for load in loads[:4]:
        load.wait()
    fold_rows(0)
    fold_rows(1)

    pl.semaphore_wait(barrier, 19)
    party_sends = []
    for k in range(1, 8):
        send = remote(pos_ref, party.at[t], p_snd.at[k - 1], p_rcv.at[t], tr(k), sigma)
        send.start()
        party_sends.append(send)
    fac_sends = []
    for k in range(1, 4):
        send = remote(fax.at[x], fax.at[x], fx_snd.at[k - 1], fx_rcv.at[x], t, xpeer(k))
        send.start()
        fac_sends.append(send)
        send = remote(faz.at[z], faz.at[z], fz_snd.at[k - 1], fz_rcv.at[z], t, zpeer(k))
        send.start()
        fac_sends.append(send)
    party[t] = pos_ref[...]

    for load in loads[4:]:
        load.wait()
    fold_rows(2)
    fold_rows(3)
    wide = mm(spot[...], fparts[...])
    high, low = halves(wide[:, :128] + wide[:, 128:])
    wide = mm(th[...], jnp.concatenate([high, low], axis=1))
    exposure = wide[:, :128] + wide[:, 128:] + mm(tl[...], high)
    etb[0] = exposure[0:128, :].T
    etb[1] = exposure[128:256, :].T

    e_all = Relay(eh, e_snd, e_rcv, y, lambda k, d: (2 * lax.rem(y + k, 4) + d, sigma))
    e_all.start(etb)

    eh[t] = etb[c]
    frows[t] = folded[t]

    fvals = jnp.concatenate([ff_ref[...].astype(F32), fd_ref[...].astype(F32), jnp.zeros((6, 1024), F32)], axis=0).astype(BF)
    lane256 = iota((1024, 256), 1)
    fidx_a = ((lane256 // 64) * 4 + x) * 64 + lane256 % 64
    fidx_b = z * 256 + lane256
    for i, fidx in enumerate((fidx_a, fidx_b)):
        picked = mm(fvals, onehot(iota((1024, 256), 0) == fidx)).astype(jnp.int32)
        pick[i] = onehot(iota((768, 256), 0) == (picked[1:2, :] - 1) * 64 + picked[0:1, :])

    for k in range(1, 8):
        src = tr(k)
        remote(pos_ref, party.at[src], p_snd.at[k - 1], p_rcv.at[src], src, sigma).wait_recv()
    for j in range(8):
        pcol[j] = upright(party[j].astype(F32))
    table = thirds(thr_ref[...]) + thirds(w_ref[...])
    table = jnp.concatenate([part.astype(F32) for part in table] + [jnp.zeros((2, 1024), F32)], axis=0).astype(BF)

    def rows_of(j, carry):
        col = pcol[j]
        rows = pl.ds(pl.multiple_of(j * 128, 128), 128)
        for i in range(8):
            same[rows, 128 * i:128 * i + 128] = onehot(col == party[i].astype(F32))
        spread = jnp.concatenate([onehot(col == lanes + 128.0 * i) for i in range(8)], axis=1)
        tw[j] = mm_nt(spread, table)
        return carry

    lax.fori_loop(0, 8, rows_of, 0)

    e_all.forward()

    def phi_of(buf, which, out_h, out_l):
        def block(q, carry):
            degree_basis(doubled(buf[q]), th, tl)
            out_h[q] = mm(th[...], pick[which]).astype(BF)
            out_l[q] = mm(tl[...], pick[which]).astype(BF)
            return carry

        lax.fori_loop(0, 4, block, 0)

    for k in range(1, 4):
        src = lax.rem(x + k, 4)
        remote(fax.at[x], fax.at[src], fx_snd.at[k - 1], fx_rcv.at[src], t, xpeer(k)).wait_recv()
    phi_of(fax, 0, pha_h, pha_l)

    e_all.finish()
    for j in range(8):
        high, low = halves(eh[j])
        ehl[128 * j:128 * j + 128, 0:128] = high
        ehl[128 * j:128 * j + 128, 128:256] = low

    def adjoint(j):
        rows = pl.ds(pl.multiple_of(j * 128, 128), 128)
        wide = mm(same[rows, :], ehl[...])
        consts = tw[j]
        shift = consts[:, 0:1] + consts[:, 1:2] + consts[:, 2:3]
        scale = consts[:, 3:4] + consts[:, 4:5] + consts[:, 5:6]
        return scale * jax.nn.sigmoid(wide[:, :128] + wide[:, 128:] - shift)

    a_all = Gather(sa, sa_snd, sa_rcv, x, lambda k, d: (2 * y + d, xpeer(k)))
    b_all = Gather(sb, sb_snd, sb_rcv, z, lambda k, d: (2 * y + d, zpeer(k)))
    for d in range(2):
        sas[d] = adjoint(2 * y + d)
    for e in (1, 0):
        d = lax.rem(c + e, 2)
        a_all.start(sas.at[d, pl.ds(0, 64)], e)
        b_all.start(sas.at[d, pl.ds(64, 64)], e)
    f_sends = []
    for k in (4, 5, 3, 2, 6, 7, 1):
        other = tr(k)
        send = remote(folded.at[other], frows.at[t], f_snd.at[k - 1], f_rcv.at[t], other, sigma)
        send.start()
        f_sends.append(send)
    sa[2 * x + c] = sas[c, 0:64, :]
    sb[2 * z + c] = sas[c, 64:128, :]
    sat[c, 2 * y] = sas[0]
    sat[c, 2 * y + 1] = sas[1]

    for k in range(2, 8):
        j = lax.rem(2 * y + k, 8)
        sat[c, j] = adjoint(j)
    sat_send = remote(sat.at[c], sat.at[c], st_snd, st_rcv, partner, sigma)
    sat_send.start()

    for i in range(8):
        ownp[:, 128 * i:128 * i + 128] = onehot(iota((256, 128), 0) + 256 * y == party[i])
    wide = mm(ownp[...], ehl[...])
    for d in range(2):
        first = pl.multiple_of(256 * y + 128 * d, 128)
        limit = upright(thr_ref[:, pl.ds(first, 128)])
        soft = jax.nn.softplus(wide[128 * d:128 * d + 128, :128] + wide[128 * d:128 * d + 128, 128:] - limit)
        xs[d] = jnp.broadcast_to(jnp.sum(soft.T, axis=0, keepdims=True), (8, 128))
    x_sends = []
    for k in range(0, 4):
        for e in range(2):
            if k == 0 and e == 0:
                continue
            d = lax.rem(c + e, 2)
            send = remote(xs.at[d], xr.at[2 * x + c], x_snd.at[2 * k + e - 1], x_rcv.at[2 * x + c], 2 * y + d, xpeer(k))
            send.start()
            x_sends.append(send)
    xr[2 * x + c] = xs[c]

    for k in range(1, 4):
        src = lax.rem(z + k, 4)
        remote(faz.at[z], faz.at[src], fz_snd.at[k - 1], fz_rcv.at[src], t, zpeer(k)).wait_recv()
    phi_of(faz, 1, phb_h, phb_l)

    low_lanes = iota((32, 128), 1) < 64

    def gradient(slots, q, out_h, out_l):
        high, low = halves(jnp.concatenate([slots[2 * q], slots[2 * q + 1]], axis=1))
        both = mm(jnp.concatenate([high, low], axis=0), out_h[q])
        return both[:64] + both[64:] + mm(high, out_l[q])

    def pack(total, dest):
        for pair in range(2):
            top = total[0:32, 128 * pair:128 * pair + 128]
            bottom = total[32:64, 128 * pair:128 * pair + 128]
            dest[2 * pair] = jnp.where(low_lanes, top, pltpu.roll(bottom, 64, 1))
            dest[2 * pair + 1] = jnp.where(low_lanes, pltpu.roll(top, 64, 1), bottom)

    total_a = jnp.zeros((64, 256), F32)
    total_b = jnp.zeros((64, 256), F32)
    for k in (0, 1, 3, 2):
        a_all.wait(k)
        b_all.wait(k)
        total_a = total_a + gradient(sa, lax.rem(x + k, 4), pha_h, pha_l)
        total_b = total_b + gradient(sb, lax.rem(z + k, 4), phb_h, phb_l)
    pack(total_a, ga)
    pack(total_b, gb)
    g_sends = []
    for k in (2, 1, 3):
        send = remote(ga.at[lax.rem(z + k, 4)], gra.at[z], ga_snd.at[k - 1], ga_rcv.at[z], t, zpeer(k))
        send.start()
        g_sends.append(send)
        send = remote(gb.at[lax.rem(x + k, 4)], grb.at[x], gb_snd.at[k - 1], gb_rcv.at[x], t, xpeer(k))
        send.start()
        g_sends.append(send)
    gra[z] = ga[z]
    grb[x] = gb[x]

    for k in range(0, 4):
        for e in range(2):
            if k == 0 and e == 0:
                continue
            d = lax.rem(c + e, 2)
            slot = 2 * lax.rem(x + k, 4) + d
            remote(xr.at[slot], xr.at[slot], x_snd.at[2 * k + e - 1], x_rcv.at[slot], 2 * y + d, xpeer(k)).wait_recv()
    part = xr[0]
    for j in range(1, 8):
        part = part + xr[j]
    xt[...] = part
    for k in range(1, 4):
        send = remote(xt, xz.at[z], x2_snd.at[k - 1], x2_rcv.at[z], t, zpeer(k))
        send.start()
        x_sends.append(send)
    xz[z] = part

    for k in range(1, 8):
        src = tr(k)
        remote(folded.at[0], frows.at[src], f_snd.at[k - 1], f_rcv.at[src], src, sigma).wait_recv()
    remote(sat.at[c], sat.at[1 - c], st_snd, st_rcv, partner, sigma).wait_recv()
    both = jnp.zeros((128, 256), F32)
    for j in range(4):
        left_h, left_l = halves(jnp.concatenate([frows[2 * j], frows[2 * j + 1]], axis=1))
        right = [jnp.concatenate([sat[0, 2 * j + i], sat[1, 2 * j + i]], axis=1) for i in range(2)]
        right_h, right_l = halves(jnp.concatenate(right, axis=0))
        both = both + mm(left_h, right_h) + mm(left_l, right_h) + mm(left_h, right_l)
    feat_out[...] = both

    row = iota((128, 128), 0)
    of_row = (row // 64) * 32 + ((row % 64) // 32) * 64 + row % 32 + 128 * t
    for j in range(16):
        takes = onehot(of_row == sot_ref[:, 128 * j:128 * j + 128])
        memt[0:128, 128 * j:128 * j + 128] = takes
        memt[128:256, 128 * j:128 * j + 128] = takes

    for k in range(1, 4):
        src = lax.rem(z + k, 4)
        remote(ga.at[0], gra.at[src], ga_snd.at[k - 1], ga_rcv.at[src], t, zpeer(k)).wait_recv()
    for k in range(1, 4):
        src = lax.rem(x + k, 4)
        remote(gb.at[0], grb.at[src], gb_snd.at[k - 1], gb_rcv.at[src], t, xpeer(k)).wait_recv()
    grad_a = (gra[0] + gra[1]) + (gra[2] + gra[3])
    grad_b = (grb[0] + grb[1]) + (grb[2] + grb[3])
    grads = jnp.concatenate([grad_a, grad_b], axis=0) * (1.0 / SCEN)
    grads = jnp.concatenate([grads, pltpu.roll(grads, 64, 1)], axis=0).T[0:64, :]
    coef_out[...] = mm(jnp.concatenate(halves(grads), axis=1), memt[...])

    for k in range(1, 4):
        src = lax.rem(z + k, 4)
        remote(xt, xz.at[src], x2_snd.at[k - 1], x2_rcv.at[src], t, zpeer(k)).wait_recv()
    whole = (xz[0] + xz[1]) + (xz[2] + xz[3])
    first = pl.multiple_of(128 * t, 128)
    xva_out[...] = w_ref[:, pl.ds(first, 128)] * whole[0:1, :] * (1.0 / SCEN)

    for send in party_sends + fac_sends + e_all.sends + f_sends + a_all.sends + b_all.sends + [sat_send] + x_sends + g_sends:
        send.wait_send()


def place_outputs(xva, coef, feat, xva_out, coef_out, feat_out, sem):
    copies = []
    for i, (src, dst) in enumerate(((coef, coef_out), (feat, feat_out), (xva, xva_out))):
        copy = pltpu.make_async_copy(src, dst, sem.at[i])
        copy.start()
        copies.append(copy)
    for copy in copies:
        copy.wait()


def local(factors, feat_factor, feat_degree, coefficients, set_of_trade, party_of_set, threshold, weight):
    vmem = pl.BlockSpec(memory_space=pltpu.VMEM)
    hbm = pl.BlockSpec(memory_space=pltpu.HBM)
    V = pltpu.VMEM
    D = pltpu.SemaphoreType.DMA
    scratch = [
        V((1, 1024), jnp.int32), V((1, 1024), jnp.int32), V((1, 2048), jnp.int32),
        V((1, 128), jnp.int32), V((1, 1024), F32), V((1, 1024), F32),
        V((1024, 2048), F32),
        V((2048, 128), BF),
        V((256, 2048), BF),
        V((2, 768, 256), BF),
        V((256, 768), BF), V((256, 768), BF),
        V((4, 64, 256), F32), V((4, 64, 256), F32),
        V((4, 256, 256), BF), V((4, 256, 256), BF), V((4, 256, 256), BF), V((4, 256, 256), BF),
        V((768, 1024), BF),
        V((1024, 256), BF),
        V((8, 128, 128), F32),
        V((8, 128, 128), F32),
        V((2, 128, 128), F32),
        V((8, 128, 128), F32),
        V((1024, 256), BF),
        V((8, 1, 128), jnp.int32),
        V((8, 128, 128), F32),
        V((1024, 1024), BF),
        V((256, 1024), BF),
        V((8, 128, 8), F32),
        V((2, 128, 128), F32),
        V((8, 64, 128), F32), V((8, 64, 128), F32),
        V((2, 8, 128, 128), F32),
        V((2, 8, 128), F32), V((8, 8, 128), F32), V((8, 128), F32), V((4, 8, 128), F32),
        V((4, 32, 128), F32), V((4, 32, 128), F32), V((4, 32, 128), F32), V((4, 32, 128), F32),
        D((8,)), D((8,)), D((7,)), D((8,)), D((3,)), D((4,)), D((3,)), D((4,)), D((14,)), D((16,)), D((7,)), D((8,)),
        D((8,)), D((8,)), D((8,)), D((8,)), D(()), D(()), D((7,)), D((8,)), D((3,)), D((4,)),
        D((3,)), D((4,)), D((3,)), D((4,)),
    ]
    shapes = (
        jax.ShapeDtypeStruct((1, 128), F32),
        jax.ShapeDtypeStruct((64, 2048), F32),
        jax.ShapeDtypeStruct((128, 256), F32),
    )
    results = pl.pallas_call(
        kernel,
        out_shape=shapes,
        in_specs=[hbm] * 8,
        out_specs=(vmem, vmem, vmem),
        scratch_shapes=scratch,
        compiler_params=pltpu.CompilerParams(collective_id=0, has_side_effects=True, vmem_limit_bytes=40 << 20),
    )(*[
        pltpu.with_memory_space_constraint(array, pltpu.HBM)
        for array in (
            coefficients, factors.T, feat_factor.reshape(1, -1), feat_degree.reshape(1, -1),
            set_of_trade.reshape(1, -1), party_of_set.reshape(1, -1), threshold.reshape(1, -1), weight.reshape(1, -1),
        )
    ])
    xva, coef_sens, feature_sens = pl.pallas_call(
        place_outputs,
        out_shape=shapes,
        in_specs=[vmem] * 3,
        out_specs=(hbm, hbm, hbm),
        scratch_shapes=[D((3,))],
        compiler_params=pltpu.CompilerParams(vmem_limit_bytes=4 << 20),
    )(*results)
    return xva.reshape(-1), coef_sens, feature_sens


def solution(mesh):
    placed = (P("scen", None), P(), P(), P(None, "trade"), P("trade"), P("trade"), P(), P())
    return jax.shard_map(
        local,
        mesh=mesh,
        in_specs=placed,
        out_specs=(P("trade"), P("scen", "trade"), P("trade", "scen")),
        check_vma=False,
    )
```

```python
import jax
import jax.numpy as jnp
from jax import lax
from jax.experimental import pallas as pl
from jax.experimental.pallas import tpu as pltpu
from jax.sharding import PartitionSpec as P

MAXDEG = 12
SCEN = 4096
MESH = pl.DeviceIdType.MESH
BF = jnp.bfloat16
F32 = jnp.float32


def mm(left, right):
    return lax.dot_general(left, right, (((1,), (0,)), ((), ())), preferred_element_type=F32)


def mm_nt(left, right):
    return lax.dot_general(left, right, (((1,), (1,)), ((), ())), preferred_element_type=F32)


def halves(value):
    high = value.astype(BF)
    return high, (value - high.astype(F32)).astype(BF)


def thirds(value):
    high = value.astype(BF)
    rest = value - high.astype(F32)
    mid = rest.astype(BF)
    return high, mid, (rest - mid.astype(F32)).astype(BF)


def iota(shape, dim):
    return lax.broadcasted_iota(jnp.int32, shape, dim)


def onehot(mask):
    return jnp.where(mask, 1.0, 0.0).astype(BF)


def upright(row):
    return jnp.broadcast_to(row, (128, 128)).T


def degree_basis(dup, out_h, out_l):
    low = iota((64, 128), 1) < 64
    for r in range(4):
        rows = slice(64 * r, 64 * r + 64)
        current = dup[rows, :]
        twice = current + current
        before = jnp.ones_like(current)
        for pair in range(MAXDEG // 2):
            after = twice * current - before
            cols = slice(128 * pair, 128 * pair + 128)
            out_h[rows, cols], out_l[rows, cols] = halves(jnp.where(low, current, after))
            if pair < MAXDEG // 2 - 1:
                before, current = after, twice * after - current


def kernel(
    coef_hbm, fac_hbm, ff_hbm, fd_hbm, sot_hbm, pos_hbm, thr_hbm, w_hbm,
    xva_out, feat_out, grads_out, memt,
    ff_ref, fd_ref, sot_ref, pos_ref, thr_ref, w_ref, cbuf,
    member, pick, th, tl, tph, tpl, fax, faz, pha_h, pha_l, phb_h, phb_l,
    spot, fparts, folded, frows, etb, eh, ehl, party, pcol, same, ownp, tw, lims, sas, sa, sb, sat,
    xs, xr, xt, xz, ga, gb, gra, grb, i_sem,
    c_sem, p_snd, p_rcv, fx_snd, fx_rcv, fz_snd, fz_rcv, e_snd, e_rcv, f_snd, f_rcv,
    sa_snd, sa_rcv, sb_snd, sb_rcv, st_snd, st_rcv, x_snd, x_rcv, x2_snd, x2_rcv,
    ga_snd, ga_rcv, gb_snd, gb_rcv,
):
    t = lax.axis_index("trade")
    sigma = lax.axis_index("scen")
    y, c = t // 2, t % 2
    z, x = sigma // 4, sigma % 4
    partner = 2 * y + 1 - c

    def remote(src, dst, snd, rcv, trade, scen):
        return pltpu.make_async_remote_copy(
            src_ref=src, dst_ref=dst, send_sem=snd, recv_sem=rcv,
            device_id=(trade, scen), device_id_type=MESH,
        )

    def tr(k):
        return lax.rem(t + k, 8)

    def xpeer(k):
        return z * 4 + lax.rem(x + k, 4)

    def zpeer(k):
        return lax.rem(z + k, 4) * 4 + x

    class Gather:
        def __init__(self, slots, snd, rcv, mine, place):
            self.slots, self.snd, self.rcv, self.mine, self.place = slots, snd, rcv, mine, place
            self.sends = []

        def put(self, src, slot, i, k, d):
            trade, scen = self.place(k, d)
            send = remote(src, self.slots.at[slot], self.snd.at[i], self.rcv.at[slot], trade, scen)
            send.start()
            self.sends.append(send)

        def start(self, src, e):
            d = lax.rem(c + e, 2)
            for i, k in enumerate((2, 1, 3) + (() if e == 0 else (0,))):
                self.put(src, 2 * self.mine + c, 4 * e + i, k, d)

        def wait(self, k):
            for e in range(2):
                if k or e:
                    slot = 2 * lax.rem(self.mine + k, 4) + lax.rem(c + e, 2)
                    trade, scen = self.place(k, lax.rem(c + e, 2))
                    here = self.slots.at[slot]
                    remote(here, here, self.snd.at[0], self.rcv.at[slot], trade, scen).wait_recv()

    class Relay(Gather):
        def half(self, slot, h):
            return self.slots.at[slot, pl.ds(64 * h, 64)]

        def put(self, src, slot, i, k, d, h):
            trade, scen = self.place(k, d)
            send = remote(src, self.half(slot, h), self.snd.at[i], self.rcv.at[2 * slot + h], trade, scen)
            send.start()
            self.sends.append(send)

        def start(self, src):
            slot = 2 * self.mine + c
            for i, (k, e) in enumerate(((1, 0), (3, 1), (1, 1), (3, 0), (0, 1))):
                d = lax.rem(c + e, 2)
                for h in range(2):
                    self.put(src.at[d, pl.ds(64 * h, 64)], slot, 2 * i + h, k, d, h)

        def wait(self, k, e, h):
            slot = 2 * lax.rem(self.mine + k, 4) + lax.rem(c + e, 2)
            trade, scen = self.place(k if k else 0, lax.rem(c + e, 2))
            here = self.half(slot, h)
            remote(here, here, self.snd.at[0], self.rcv.at[2 * slot + h], trade, scen).wait_recv()
            return slot

        def forward(self):
            for h in range(2):
                slot = self.wait(3, 0, h)
                self.put(self.half(slot, h), slot, 10 + h, 1, c, h)
                slot = self.wait(1, 1, h)
                self.put(self.half(slot, h), slot, 12 + h, 3, c, h)

        def near(self):
            for h in range(2):
                for k, e in ((0, 1), (3, 1), (1, 0)):
                    self.wait(k, e, h)

        def far(self):
            for h in range(2):
                for e in range(2):
                    self.wait(2, e, h)

    smalls = []
    for i, (src, dst) in enumerate((
        (sot_hbm, sot_ref), (ff_hbm, ff_ref), (fd_hbm, fd_ref), (fac_hbm, fax.at[x]), (fac_hbm, faz.at[z]),
        (pos_hbm, pos_ref), (thr_hbm, thr_ref), (w_hbm, w_ref),
    )):
        small = pltpu.make_async_copy(src, dst, i_sem.at[i])
        small.start()
        smalls.append(small)
    loads = []
    for i in range(8):
        rows = pl.ds(128 * i, 128)
        loads.append(pltpu.make_async_copy(coef_hbm.at[rows], cbuf.at[rows], c_sem.at[i]))
    for load in loads:
        load.start(priority=1)
    barrier = pltpu.get_barrier_semaphore()
    for k in range(1, 8):
        pl.semaphore_signal(barrier, inc=1, device_id=(tr(k), sigma), device_id_type=MESH)
    for k in range(1, 4):
        for d in range(2):
            pl.semaphore_signal(barrier, inc=1, device_id=(2 * y + d, xpeer(k)), device_id_type=MESH)
            pl.semaphore_signal(barrier, inc=1, device_id=(2 * y + d, zpeer(k)), device_id_type=MESH)

    for small in smalls:
        small.wait()
    base = (128 * t).astype(F32)
    lanes = iota((128, 128), 1).astype(F32)
    for j in range(16):
        col = upright(sot_ref[:, 128 * j:128 * j + 128].astype(F32) - base)
        member[128 * j:128 * j + 128, :] = onehot(col == lanes)

    def doubled(facts):
        return jnp.concatenate([facts, facts], axis=0).T

    degree_basis(doubled(fax[x]), th, tl)

    keys = (fd_ref[...] - 1) * 64 + ff_ref[...]
    for i in range(8):
        cols = slice(128 * i, 128 * i + 128)
        spot[:, cols] = onehot(iota((768, 128), 0) == keys[:, cols])

    def fold_rows(i):
        rows = slice(256 * i, 256 * i + 256)
        high, low = halves(cbuf[rows, :])
        fold = mm(high, member[...]) + mm(low, member[...])
        folded[2 * i] = fold[:128, :]
        folded[2 * i + 1] = fold[128:, :]
        high, low = halves(fold)
        fparts[rows, 0:128] = high
        fparts[rows, 128:256] = low

    for load in loads[:4]:
        load.wait()
    fold_rows(0)
    fold_rows(1)

    pl.semaphore_wait(barrier, 19)
    party_sends = []
    for k in range(1, 8):
        send = remote(pos_ref, party.at[t], p_snd.at[k - 1], p_rcv.at[t], tr(k), sigma)
        send.start()
        party_sends.append(send)
    fac_sends = []
    for k in range(1, 4):
        send = remote(fax.at[x], fax.at[x], fx_snd.at[k - 1], fx_rcv.at[x], t, xpeer(k))
        send.start()
        fac_sends.append(send)
        send = remote(faz.at[z], faz.at[z], fz_snd.at[k - 1], fz_rcv.at[z], t, zpeer(k))
        send.start()
        fac_sends.append(send)
    party[t] = pos_ref[...]

    for load in loads[4:]:
        load.wait()
    fold_rows(2)
    fold_rows(3)
    wide = mm(spot[...], fparts[...])
    high, low = halves(wide[:, :128] + wide[:, 128:])
    wide = mm(th[...], jnp.concatenate([high, low], axis=1))
    exposure = wide[:, :128] + wide[:, 128:] + mm(tl[...], high)
    etb[0] = exposure[0:128, :].T
    etb[1] = exposure[128:256, :].T

    e_all = Relay(eh, e_snd, e_rcv, y, lambda k, d: (2 * lax.rem(y + k, 4) + d, sigma))
    e_all.start(etb)

    eh[t] = etb[c]
    frows[t] = folded[t]

    fvals = jnp.concatenate([ff_ref[...].astype(F32), fd_ref[...].astype(F32), jnp.zeros((6, 1024), F32)], axis=0).astype(BF)
    lane256 = iota((1024, 256), 1)
    fidx_a = ((lane256 // 64) * 4 + x) * 64 + lane256 % 64
    fidx_b = z * 256 + lane256
    for i, fidx in enumerate((fidx_a, fidx_b)):
        picked = mm(fvals, onehot(iota((1024, 256), 0) == fidx)).astype(jnp.int32)
        pick[i] = onehot(iota((768, 256), 0) == (picked[1:2, :] - 1) * 64 + picked[0:1, :])

    for k in range(1, 8):
        src = tr(k)
        remote(pos_ref, party.at[src], p_snd.at[k - 1], p_rcv.at[src], src, sigma).wait_recv()
    for j in range(8):
        pcol[j] = upright(party[j].astype(F32))
    table = thirds(thr_ref[...]) + thirds(w_ref[...])
    table = jnp.concatenate([part.astype(F32) for part in table] + [jnp.zeros((2, 1024), F32)], axis=0).astype(BF)

    def rows_of(j, carry):
        col = pcol[j]
        rows = pl.ds(pl.multiple_of(j * 128, 128), 128)
        for i in range(8):
            same[rows, 128 * i:128 * i + 128] = onehot(col == party[i].astype(F32))
        spread = jnp.concatenate([onehot(col == lanes + 128.0 * i) for i in range(8)], axis=1)
        tw[j] = mm_nt(spread, table)
        return carry

    lax.fori_loop(0, 8, rows_of, 0)

    def limits(j):
        consts = tw[j]
        return consts[:, 0:1] + consts[:, 1:2] + consts[:, 2:3], consts[:, 3:4] + consts[:, 4:5] + consts[:, 5:6]

    for d in range(2):
        rows = slice(128 * d, 128 * d + 128)
        for i, column in enumerate(limits(2 * y + d)):
            lims[i, rows, :] = jnp.broadcast_to(column, (128, 128))

    e_all.forward()

    def phi_of(buf, which, mine, out_h, out_l):
        out_h[mine] = mm(th[...], pick[which]).astype(BF)
        out_l[mine] = mm(tl[...], pick[which]).astype(BF)
        for k in range(1, 4):
            q = lax.rem(mine + k, 4)
            degree_basis(doubled(buf[q]), tph.at[k - 1], tpl.at[k - 1])
            out_h[q] = mm(tph[k - 1], pick[which]).astype(BF)
            out_l[q] = mm(tpl[k - 1], pick[which]).astype(BF)

    for k in range(1, 4):
        src = lax.rem(x + k, 4)
        remote(fax.at[x], fax.at[src], fx_snd.at[k - 1], fx_rcv.at[src], t, xpeer(k)).wait_recv()
    phi_of(fax, 0, x, pha_h, pha_l)

    def split(m):
        for d in range(2):
            rows = pl.ds(pl.multiple_of(256 * m + 128 * d, 128), 128)
            ehl[rows, 0:128], ehl[rows, 128:256] = halves(eh[2 * m + d])

    chip = pl.ds(pl.multiple_of(256 * y, 256), 256)

    def netted(m):
        cols = pl.ds(pl.multiple_of(256 * m, 256), 256)
        return mm(same[chip, cols], ehl[cols, :])

    e_all.near()
    wide = jnp.zeros((256, 256), F32)
    for k in (0, 1, 3):
        m = lax.rem(y + k, 4)
        split(m)
        wide = wide + netted(m)
    net = wide[:, :128] + wide[:, 128:] - lims[0]
    e_all.far()
    m = lax.rem(y + 2, 4)
    split(m)
    wide = netted(m)
    sas[...] = (lims[1] * jax.nn.sigmoid(net + (wide[:, :128] + wide[:, 128:]))).reshape(2, 128, 128)

    def adjoint(j):
        rows = pl.ds(pl.multiple_of(j * 128, 128), 128)
        wide = mm(same[rows, :], ehl[...])
        shift, scale = limits(j)
        return scale * jax.nn.sigmoid(wide[:, :128] + wide[:, 128:] - shift)

    a_all = Gather(sa, sa_snd, sa_rcv, x, lambda k, d: (2 * y + d, xpeer(k)))
    b_all = Gather(sb, sb_snd, sb_rcv, z, lambda k, d: (2 * y + d, zpeer(k)))
    for e in (1, 0):
        d = lax.rem(c + e, 2)
        a_all.start(sas.at[d, pl.ds(0, 64)], e)
        b_all.start(sas.at[d, pl.ds(64, 64)], e)
    f_sends = []
    for k in (4, 5, 3, 2, 6, 7, 1):
        other = tr(k)
        send = remote(folded.at[other], frows.at[t], f_snd.at[k - 1], f_rcv.at[t], other, sigma)
        send.start()
        f_sends.append(send)
    sa[2 * x + c] = sas[c, 0:64, :]
    sb[2 * z + c] = sas[c, 64:128, :]
    sat[c, 2 * y] = sas[0]
    sat[c, 2 * y + 1] = sas[1]

    for k in range(2, 8):
        j = lax.rem(2 * y + k, 8)
        sat[c, j] = adjoint(j)
    sat_send = remote(sat.at[c], sat.at[c], st_snd, st_rcv, partner, sigma)
    sat_send.start()

    for i in range(8):
        ownp[:, 128 * i:128 * i + 128] = onehot(iota((256, 128), 0) + 256 * y == party[i])
    wide = mm(ownp[...], ehl[...])
    for d in range(2):
        first = pl.multiple_of(256 * y + 128 * d, 128)
        limit = upright(thr_ref[:, pl.ds(first, 128)])
        soft = jax.nn.softplus(wide[128 * d:128 * d + 128, :128] + wide[128 * d:128 * d + 128, 128:] - limit)
        xs[d] = jnp.broadcast_to(jnp.sum(soft.T, axis=0, keepdims=True), (8, 128))
    x_sends = []
    for k in range(0, 4):
        for e in range(2):
            if k == 0 and e == 0:
                continue
            d = lax.rem(c + e, 2)
            send = remote(xs.at[d], xr.at[2 * x + c], x_snd.at[2 * k + e - 1], x_rcv.at[2 * x + c], 2 * y + d, xpeer(k))
            send.start()
            x_sends.append(send)
    xr[2 * x + c] = xs[c]

    for k in range(1, 4):
        src = lax.rem(z + k, 4)
        remote(faz.at[z], faz.at[src], fz_snd.at[k - 1], fz_rcv.at[src], t, zpeer(k)).wait_recv()
    phi_of(faz, 1, z, phb_h, phb_l)

    low_lanes = iota((32, 128), 1) < 64

    def gradient(slots, q, out_h, out_l):
        high, low = halves(jnp.concatenate([slots[2 * q], slots[2 * q + 1]], axis=1))
        both = mm(jnp.concatenate([high, low], axis=0), out_h[q])
        return both[:64] + both[64:] + mm(high, out_l[q])

    def pack(total, dest):
        for pair in range(2):
            top = total[0:32, 128 * pair:128 * pair + 128]
            bottom = total[32:64, 128 * pair:128 * pair + 128]
            dest[2 * pair] = jnp.where(low_lanes, top, pltpu.roll(bottom, 64, 1))
            dest[2 * pair + 1] = jnp.where(low_lanes, pltpu.roll(top, 64, 1), bottom)

    total_a = jnp.zeros((64, 256), F32)
    total_b = jnp.zeros((64, 256), F32)
    for k in (0, 1, 3, 2):
        a_all.wait(k)
        b_all.wait(k)
        total_a = total_a + gradient(sa, lax.rem(x + k, 4), pha_h, pha_l)
        total_b = total_b + gradient(sb, lax.rem(z + k, 4), phb_h, phb_l)
    pack(total_a, ga)
    pack(total_b, gb)
    g_sends = []
    for k in (2, 1, 3):
        send = remote(ga.at[lax.rem(z + k, 4)], gra.at[z], ga_snd.at[k - 1], ga_rcv.at[z], t, zpeer(k))
        send.start()
        g_sends.append(send)
        send = remote(gb.at[lax.rem(x + k, 4)], grb.at[x], gb_snd.at[k - 1], gb_rcv.at[x], t, xpeer(k))
        send.start()
        g_sends.append(send)
    gra[z] = ga[z]
    grb[x] = gb[x]

    for k in range(0, 4):
        for e in range(2):
            if k == 0 and e == 0:
                continue
            d = lax.rem(c + e, 2)
            slot = 2 * lax.rem(x + k, 4) + d
            remote(xr.at[slot], xr.at[slot], x_snd.at[2 * k + e - 1], x_rcv.at[slot], 2 * y + d, xpeer(k)).wait_recv()
    part = xr[0]
    for j in range(1, 8):
        part = part + xr[j]
    xt[...] = part
    for k in range(1, 4):
        send = remote(xt, xz.at[z], x2_snd.at[k - 1], x2_rcv.at[z], t, zpeer(k))
        send.start()
        x_sends.append(send)
    xz[z] = part

    for k in range(1, 8):
        src = tr(k)
        remote(folded.at[0], frows.at[src], f_snd.at[k - 1], f_rcv.at[src], src, sigma).wait_recv()
    remote(sat.at[c], sat.at[1 - c], st_snd, st_rcv, partner, sigma).wait_recv()
    both = jnp.zeros((128, 256), F32)
    for j in range(4):
        left_h, left_l = halves(jnp.concatenate([frows[2 * j], frows[2 * j + 1]], axis=1))
        right = [jnp.concatenate([sat[0, 2 * j + i], sat[1, 2 * j + i]], axis=1) for i in range(2)]
        right_h, right_l = halves(jnp.concatenate(right, axis=0))
        both = both + mm(left_h, right_h) + mm(left_l, right_h) + mm(left_h, right_l)
    feat_out[...] = both

    row = iota((128, 128), 0)
    of_row = (row // 64) * 32 + ((row % 64) // 32) * 64 + row % 32 + 128 * t
    for j in range(16):
        takes = onehot(of_row == sot_ref[:, 128 * j:128 * j + 128])
        memt[0:128, 128 * j:128 * j + 128] = takes
        memt[128:256, 128 * j:128 * j + 128] = takes

    for k in range(1, 4):
        src = lax.rem(z + k, 4)
        remote(ga.at[0], gra.at[src], ga_snd.at[k - 1], ga_rcv.at[src], t, zpeer(k)).wait_recv()
    for k in range(1, 4):
        src = lax.rem(x + k, 4)
        remote(gb.at[0], grb.at[src], gb_snd.at[k - 1], gb_rcv.at[src], t, xpeer(k)).wait_recv()
    grad_a = (gra[0] + gra[1]) + (gra[2] + gra[3])
    grad_b = (grb[0] + grb[1]) + (grb[2] + grb[3])
    grads = jnp.concatenate([grad_a, grad_b], axis=0) * (1.0 / SCEN)
    grads = jnp.concatenate([grads, pltpu.roll(grads, 64, 1)], axis=0).T[0:64, :]
    grads_out[...] = jnp.concatenate(halves(grads), axis=1)

    for k in range(1, 4):
        src = lax.rem(z + k, 4)
        remote(xt, xz.at[src], x2_snd.at[k - 1], x2_rcv.at[src], t, zpeer(k)).wait_recv()
    whole = (xz[0] + xz[1]) + (xz[2] + xz[3])
    first = pl.multiple_of(128 * t, 128)
    xva_out[...] = w_ref[:, pl.ds(first, 128)] * whole[0:1, :] * (1.0 / SCEN)

    for send in party_sends + fac_sends + e_all.sends + f_sends + a_all.sends + b_all.sends + [sat_send] + x_sends + g_sends:
        send.wait_send()


def place_outputs(xva, feat, grads, memt, xva_out, coef_out, feat_out, coef, sem):
    copies = [pltpu.make_async_copy(feat, feat_out, sem.at[4]), pltpu.make_async_copy(xva, xva_out, sem.at[5])]
    for copy in copies:
        copy.start()
    for i in range(4):
        cols = pl.ds(512 * i, 512)
        coef[i] = mm(grads[...], memt[:, 512 * i:512 * i + 512])
        copy = pltpu.make_async_copy(coef.at[i], coef_out.at[:, cols], sem.at[i])
        copy.start()
        copies.append(copy)
    for copy in copies:
        copy.wait()


def local(factors, feat_factor, feat_degree, coefficients, set_of_trade, party_of_set, threshold, weight):
    vmem = pl.BlockSpec(memory_space=pltpu.VMEM)
    hbm = pl.BlockSpec(memory_space=pltpu.HBM)
    V = pltpu.VMEM
    D = pltpu.SemaphoreType.DMA
    scratch = [
        V((1, 1024), jnp.int32), V((1, 1024), jnp.int32), V((1, 2048), jnp.int32),
        V((1, 128), jnp.int32), V((1, 1024), F32), V((1, 1024), F32),
        V((1024, 2048), F32),
        V((2048, 128), BF),
        V((2, 768, 256), BF),
        V((256, 768), BF), V((256, 768), BF),
        V((3, 256, 768), BF), V((3, 256, 768), BF),
        V((4, 64, 256), F32), V((4, 64, 256), F32),
        V((4, 256, 256), BF), V((4, 256, 256), BF), V((4, 256, 256), BF), V((4, 256, 256), BF),
        V((768, 1024), BF),
        V((1024, 256), BF),
        V((8, 128, 128), F32),
        V((8, 128, 128), F32),
        V((2, 128, 128), F32),
        V((8, 128, 128), F32),
        V((1024, 256), BF),
        V((8, 1, 128), jnp.int32),
        V((8, 128, 128), F32),
        V((1024, 1024), BF),
        V((256, 1024), BF),
        V((8, 128, 8), F32),
        V((2, 256, 128), F32),
        V((2, 128, 128), F32),
        V((8, 64, 128), F32), V((8, 64, 128), F32),
        V((2, 8, 128, 128), F32),
        V((2, 8, 128), F32), V((8, 8, 128), F32), V((8, 128), F32), V((4, 8, 128), F32),
        V((4, 32, 128), F32), V((4, 32, 128), F32), V((4, 32, 128), F32), V((4, 32, 128), F32),
        D((8,)), D((8,)), D((7,)), D((8,)), D((3,)), D((4,)), D((3,)), D((4,)), D((14,)), D((16,)), D((7,)), D((8,)),
        D((8,)), D((8,)), D((8,)), D((8,)), D(()), D(()), D((7,)), D((8,)), D((3,)), D((4,)),
        D((3,)), D((4,)), D((3,)), D((4,)),
    ]
    xva_shape = jax.ShapeDtypeStruct((1, 128), F32)
    coef_shape = jax.ShapeDtypeStruct((64, 2048), F32)
    feat_shape = jax.ShapeDtypeStruct((128, 256), F32)
    results = pl.pallas_call(
        kernel,
        out_shape=(xva_shape, feat_shape, jax.ShapeDtypeStruct((64, 256), BF), jax.ShapeDtypeStruct((256, 2048), BF)),
        in_specs=[hbm] * 8,
        out_specs=(vmem, vmem, vmem, vmem),
        scratch_shapes=scratch,
        compiler_params=pltpu.CompilerParams(collective_id=0, has_side_effects=True, vmem_limit_bytes=40 << 20),
    )(*[
        pltpu.with_memory_space_constraint(array, pltpu.HBM)
        for array in (
            coefficients, factors.T, feat_factor.reshape(1, -1), feat_degree.reshape(1, -1),
            set_of_trade.reshape(1, -1), party_of_set.reshape(1, -1), threshold.reshape(1, -1), weight.reshape(1, -1),
        )
    ])
    xva, coef_sens, feature_sens = pl.pallas_call(
        place_outputs,
        out_shape=(xva_shape, coef_shape, feat_shape),
        in_specs=[vmem] * 4,
        out_specs=(hbm, hbm, hbm),
        scratch_shapes=[V((4, 64, 512), F32), D((6,))],
        compiler_params=pltpu.CompilerParams(vmem_limit_bytes=4 << 20),
    )(*results)
    return xva.reshape(-1), coef_sens, feature_sens


def solution(mesh):
    placed = (P("scen", None), P(), P(), P(None, "trade"), P("trade"), P("trade"), P(), P())
    return jax.shard_map(
        local,
        mesh=mesh,
        in_specs=placed,
        out_specs=(P("trade"), P("scen", "trade"), P("trade", "scen")),
        check_vma=False,
    )
```

```python
import jax
import jax.numpy as jnp
from jax import lax
from jax.experimental import pallas as pl
from jax.experimental.pallas import tpu as pltpu
from jax.sharding import PartitionSpec as P

MAXDEG = 12
SCEN = 4096
MESH = pl.DeviceIdType.MESH
BF = jnp.bfloat16
F32 = jnp.float32


def mm(left, right):
    return lax.dot_general(left, right, (((1,), (0,)), ((), ())), preferred_element_type=F32)


def mm_nt(left, right):
    return lax.dot_general(left, right, (((1,), (1,)), ((), ())), preferred_element_type=F32)


def halves(value):
    high = value.astype(BF)
    return high, (value - high.astype(F32)).astype(BF)


def thirds(value):
    high = value.astype(BF)
    rest = value - high.astype(F32)
    mid = rest.astype(BF)
    return high, mid, (rest - mid.astype(F32)).astype(BF)


def iota(shape, dim):
    return lax.broadcasted_iota(jnp.int32, shape, dim)


def onehot(mask):
    return jnp.where(mask, 1.0, 0.0).astype(BF)


def upright(row):
    return jnp.broadcast_to(row, (128, 128)).T


def degree_basis(dup, out_h, out_l):
    low = iota((64, 128), 1) < 64
    for r in range(4):
        rows = slice(64 * r, 64 * r + 64)
        current = dup[rows, :]
        twice = current + current
        before = jnp.ones_like(current)
        for pair in range(MAXDEG // 2):
            after = twice * current - before
            cols = slice(128 * pair, 128 * pair + 128)
            out_h[rows, cols], out_l[rows, cols] = halves(jnp.where(low, current, after))
            if pair < MAXDEG // 2 - 1:
                before, current = after, twice * after - current


def kernel(
    coef_hbm, fac_hbm, ff_hbm, fd_hbm, sot_hbm, pos_hbm, thr_hbm, w_hbm,
    xva_out, feat_out, grads_out, memt,
    ff_ref, fd_ref, sot_ref, pos_ref, thr_ref, w_ref, cbuf,
    member, pick, th, tl, tph, tpl, fax, faz, pha_h, pha_l, phb_h, phb_l,
    spot, fparts, folded, frows, etb, eh, ehl, party, pcol, same, ownp, tw, lims, sas, sa, sb, sat,
    xs, xr, xt, xz, ga, gb, gra, grb, i_sem,
    c_sem, p_snd, p_rcv, fx_snd, fx_rcv, fz_snd, fz_rcv, e_snd, e_rcv, f_snd, f_rcv,
    sa_snd, sa_rcv, sb_snd, sb_rcv, st_snd, st_rcv, x_snd, x_rcv, x2_snd, x2_rcv,
    ga_snd, ga_rcv, gb_snd, gb_rcv,
):
    t = lax.axis_index("trade")
    sigma = lax.axis_index("scen")
    y, c = t // 2, t % 2
    z, x = sigma // 4, sigma % 4
    partner = 2 * y + 1 - c

    def remote(src, dst, snd, rcv, trade, scen):
        return pltpu.make_async_remote_copy(
            src_ref=src, dst_ref=dst, send_sem=snd, recv_sem=rcv,
            device_id=(trade, scen), device_id_type=MESH,
        )

    def tr(k):
        return lax.rem(t + k, 8)

    def xpeer(k):
        return z * 4 + lax.rem(x + k, 4)

    def zpeer(k):
        return lax.rem(z + k, 4) * 4 + x

    class Gather:
        def __init__(self, slots, snd, rcv, mine, place):
            self.slots, self.snd, self.rcv, self.mine, self.place = slots, snd, rcv, mine, place
            self.sends = []

        def put(self, src, slot, i, k, d):
            trade, scen = self.place(k, d)
            send = remote(src, self.slots.at[slot], self.snd.at[i], self.rcv.at[slot], trade, scen)
            send.start()
            self.sends.append(send)

        def start(self, src, e):
            d = lax.rem(c + e, 2)
            for i, k in enumerate((2, 1, 3) + (() if e == 0 else (0,))):
                self.put(src, 2 * self.mine + c, 4 * e + i, k, d)

        def wait(self, k):
            for e in range(2):
                if k or e:
                    slot = 2 * lax.rem(self.mine + k, 4) + lax.rem(c + e, 2)
                    trade, scen = self.place(k, lax.rem(c + e, 2))
                    here = self.slots.at[slot]
                    remote(here, here, self.snd.at[0], self.rcv.at[slot], trade, scen).wait_recv()

    class Relay(Gather):
        def half(self, slot, h):
            return self.slots.at[slot, pl.ds(64 * h, 64)]

        def put(self, src, slot, i, k, d, h):
            trade, scen = self.place(k, d)
            send = remote(src, self.half(slot, h), self.snd.at[i], self.rcv.at[2 * slot + h], trade, scen)
            send.start()
            self.sends.append(send)

        def start(self, src):
            slot = 2 * self.mine + c
            for i, (k, e) in enumerate(((1, 0), (3, 1), (1, 1), (3, 0), (0, 1))):
                d = lax.rem(c + e, 2)
                for h in range(2):
                    self.put(src.at[d, pl.ds(64 * h, 64)], slot, 2 * i + h, k, d, h)

        def wait(self, k, e, h):
            slot = 2 * lax.rem(self.mine + k, 4) + lax.rem(c + e, 2)
            trade, scen = self.place(k if k else 0, lax.rem(c + e, 2))
            here = self.half(slot, h)
            remote(here, here, self.snd.at[0], self.rcv.at[2 * slot + h], trade, scen).wait_recv()
            return slot

        def forward(self):
            for h in range(2):
                slot = self.wait(3, 0, h)
                self.put(self.half(slot, h), slot, 10 + h, 1, c, h)
                slot = self.wait(1, 1, h)
                self.put(self.half(slot, h), slot, 12 + h, 3, c, h)

        def near(self):
            for h in range(2):
                for k, e in ((0, 1), (3, 1), (1, 0)):
                    self.wait(k, e, h)

        def far(self):
            for h in range(2):
                for e in range(2):
                    self.wait(2, e, h)

    smalls = []
    for i, (src, dst) in enumerate((
        (sot_hbm, sot_ref), (ff_hbm, ff_ref), (fd_hbm, fd_ref), (fac_hbm, fax.at[x]), (fac_hbm, faz.at[z]),
        (pos_hbm, pos_ref), (thr_hbm, thr_ref), (w_hbm, w_ref),
    )):
        small = pltpu.make_async_copy(src, dst, i_sem.at[i])
        small.start()
        smalls.append(small)
    loads = []
    for i in range(8):
        rows = pl.ds(128 * i, 128)
        loads.append(pltpu.make_async_copy(coef_hbm.at[rows], cbuf.at[rows], c_sem.at[i]))
    for load in loads:
        load.start(priority=1)
    barrier = pltpu.get_barrier_semaphore()
    for k in range(1, 8):
        pl.semaphore_signal(barrier, inc=1, device_id=(tr(k), sigma), device_id_type=MESH)
    for k in range(1, 4):
        for d in range(2):
            pl.semaphore_signal(barrier, inc=1, device_id=(2 * y + d, xpeer(k)), device_id_type=MESH)
            pl.semaphore_signal(barrier, inc=1, device_id=(2 * y + d, zpeer(k)), device_id_type=MESH)

    for small in smalls:
        small.wait()
    base = (128 * t).astype(F32)
    lanes = iota((128, 128), 1).astype(F32)
    for j in range(16):
        col = upright(sot_ref[:, 128 * j:128 * j + 128].astype(F32) - base)
        member[128 * j:128 * j + 128, :] = onehot(col == lanes)

    def doubled(facts):
        return jnp.concatenate([facts, facts], axis=0).T

    degree_basis(doubled(fax[x]), th, tl)

    keys = (fd_ref[...] - 1) * 64 + ff_ref[...]
    for i in range(8):
        cols = slice(128 * i, 128 * i + 128)
        spot[:, cols] = onehot(iota((768, 128), 0) == keys[:, cols])

    def fold_rows(i):
        rows = slice(256 * i, 256 * i + 256)
        high, low = halves(cbuf[rows, :])
        fold = mm(high, member[...]) + mm(low, member[...])
        folded[2 * i] = fold[:128, :]
        folded[2 * i + 1] = fold[128:, :]
        high, low = halves(fold)
        fparts[rows, 0:128] = high
        fparts[rows, 128:256] = low

    for load in loads[:4]:
        load.wait()
    fold_rows(0)
    fold_rows(1)

    pl.semaphore_wait(barrier, 19)
    party_sends = []
    for k in range(1, 8):
        send = remote(pos_ref, party.at[t], p_snd.at[k - 1], p_rcv.at[t], tr(k), sigma)
        send.start()
        party_sends.append(send)
    fac_sends = []
    for k in range(1, 4):
        send = remote(fax.at[x], fax.at[x], fx_snd.at[k - 1], fx_rcv.at[x], t, xpeer(k))
        send.start()
        fac_sends.append(send)
        send = remote(faz.at[z], faz.at[z], fz_snd.at[k - 1], fz_rcv.at[z], t, zpeer(k))
        send.start()
        fac_sends.append(send)
    party[t] = pos_ref[...]

    for load in loads[4:]:
        load.wait()
    fold_rows(2)
    fold_rows(3)
    wide = mm(spot[...], fparts[...])
    high, low = halves(wide[:, :128] + wide[:, 128:])
    wide = mm(th[...], jnp.concatenate([high, low], axis=1))
    exposure = wide[:, :128] + wide[:, 128:] + mm(tl[...], high)
    etb[0] = exposure[0:128, :].T
    etb[1] = exposure[128:256, :].T

    e_all = Relay(eh, e_snd, e_rcv, y, lambda k, d: (2 * lax.rem(y + k, 4) + d, sigma))
    e_all.start(etb)

    eh[t] = etb[c]
    frows[t] = folded[t]

    for k in range(1, 8):
        src = tr(k)
        remote(pos_ref, party.at[src], p_snd.at[k - 1], p_rcv.at[src], src, sigma).wait_recv()
    for j in range(8):
        pcol[j] = upright(party[j].astype(F32))
    table = thirds(thr_ref[...]) + thirds(w_ref[...])
    table = jnp.concatenate([part.astype(F32) for part in table] + [jnp.zeros((2, 1024), F32)], axis=0).astype(BF)

    def rows_of(j, carry):
        col = pcol[j]
        rows = pl.ds(pl.multiple_of(j * 128, 128), 128)
        for i in range(8):
            same[rows, 128 * i:128 * i + 128] = onehot(col == party[i].astype(F32))
        spread = jnp.concatenate([onehot(col == lanes + 128.0 * i) for i in range(8)], axis=1)
        tw[j] = mm_nt(spread, table)
        return carry

    lax.fori_loop(0, 8, rows_of, 0)

    e_all.forward()

    fvals = jnp.concatenate([ff_ref[...].astype(F32), fd_ref[...].astype(F32), jnp.zeros((6, 1024), F32)], axis=0).astype(BF)
    lane256 = iota((1024, 256), 1)
    fidx_a = ((lane256 // 64) * 4 + x) * 64 + lane256 % 64
    fidx_b = z * 256 + lane256
    for i, fidx in enumerate((fidx_a, fidx_b)):
        picked = mm(fvals, onehot(iota((1024, 256), 0) == fidx)).astype(jnp.int32)
        pick[i] = onehot(iota((768, 256), 0) == (picked[1:2, :] - 1) * 64 + picked[0:1, :])

    def limits(j):
        consts = tw[j]
        return consts[:, 0:1] + consts[:, 1:2] + consts[:, 2:3], consts[:, 3:4] + consts[:, 4:5] + consts[:, 5:6]

    for d in range(2):
        rows = slice(128 * d, 128 * d + 128)
        for i, column in enumerate(limits(2 * y + d)):
            lims[i, rows, :] = jnp.broadcast_to(column, (128, 128))

    def phi_of(buf, which, mine, out_h, out_l):
        out_h[mine] = mm(th[...], pick[which]).astype(BF)
        out_l[mine] = mm(tl[...], pick[which]).astype(BF)
        for k in range(1, 4):
            q = lax.rem(mine + k, 4)
            degree_basis(doubled(buf[q]), tph.at[k - 1], tpl.at[k - 1])
            out_h[q] = mm(tph[k - 1], pick[which]).astype(BF)
            out_l[q] = mm(tpl[k - 1], pick[which]).astype(BF)

    for k in range(1, 4):
        src = lax.rem(x + k, 4)
        remote(fax.at[x], fax.at[src], fx_snd.at[k - 1], fx_rcv.at[src], t, xpeer(k)).wait_recv()
    phi_of(fax, 0, x, pha_h, pha_l)

    def split(m):
        for d in range(2):
            rows = pl.ds(pl.multiple_of(256 * m + 128 * d, 128), 128)
            ehl[rows, 0:128], ehl[rows, 128:256] = halves(eh[2 * m + d])

    chip = pl.ds(pl.multiple_of(256 * y, 256), 256)

    def netted(m):
        cols = pl.ds(pl.multiple_of(256 * m, 256), 256)
        return mm(same[chip, cols], ehl[cols, :])

    e_all.near()
    wide = jnp.zeros((256, 256), F32)
    for k in (0, 1, 3):
        m = lax.rem(y + k, 4)
        split(m)
        wide = wide + netted(m)
    net = wide[:, :128] + wide[:, 128:] - lims[0]
    e_all.far()
    m = lax.rem(y + 2, 4)
    split(m)
    wide = netted(m)
    sas[...] = (lims[1] * jax.nn.sigmoid(net + (wide[:, :128] + wide[:, 128:]))).reshape(2, 128, 128)

    def adjoint(j):
        rows = pl.ds(pl.multiple_of(j * 128, 128), 128)
        wide = mm(same[rows, :], ehl[...])
        shift, scale = limits(j)
        return scale * jax.nn.sigmoid(wide[:, :128] + wide[:, 128:] - shift)

    a_all = Gather(sa, sa_snd, sa_rcv, x, lambda k, d: (2 * y + d, xpeer(k)))
    b_all = Gather(sb, sb_snd, sb_rcv, z, lambda k, d: (2 * y + d, zpeer(k)))
    for e in (1, 0):
        d = lax.rem(c + e, 2)
        a_all.start(sas.at[d, pl.ds(0, 64)], e)
        b_all.start(sas.at[d, pl.ds(64, 64)], e)
    f_sends = []
    for k in (4, 5, 3, 2, 6, 7, 1):
        other = tr(k)
        send = remote(folded.at[other], frows.at[t], f_snd.at[k - 1], f_rcv.at[t], other, sigma)
        send.start()
        f_sends.append(send)
    sa[2 * x + c] = sas[c, 0:64, :]
    sb[2 * z + c] = sas[c, 64:128, :]
    sat[c, 2 * y] = sas[0]
    sat[c, 2 * y + 1] = sas[1]

    for k in range(2, 8):
        j = lax.rem(2 * y + k, 8)
        sat[c, j] = adjoint(j)
    sat_send = remote(sat.at[c], sat.at[c], st_snd, st_rcv, partner, sigma)
    sat_send.start()

    for i in range(8):
        ownp[:, 128 * i:128 * i + 128] = onehot(iota((256, 128), 0) + 256 * y == party[i])
    wide = mm(ownp[...], ehl[...])
    for d in range(2):
        first = pl.multiple_of(256 * y + 128 * d, 128)
        limit = upright(thr_ref[:, pl.ds(first, 128)])
        soft = jax.nn.softplus(wide[128 * d:128 * d + 128, :128] + wide[128 * d:128 * d + 128, 128:] - limit)
        xs[d] = jnp.broadcast_to(jnp.sum(soft.T, axis=0, keepdims=True), (8, 128))
    x_sends = []
    for k in range(0, 4):
        for e in range(2):
            if k == 0 and e == 0:
                continue
            d = lax.rem(c + e, 2)
            send = remote(xs.at[d], xr.at[2 * x + c], x_snd.at[2 * k + e - 1], x_rcv.at[2 * x + c], 2 * y + d, xpeer(k))
            send.start()
            x_sends.append(send)
    xr[2 * x + c] = xs[c]

    for k in range(1, 4):
        src = lax.rem(z + k, 4)
        remote(faz.at[z], faz.at[src], fz_snd.at[k - 1], fz_rcv.at[src], t, zpeer(k)).wait_recv()
    phi_of(faz, 1, z, phb_h, phb_l)

    low_lanes = iota((32, 128), 1) < 64

    def gradient(slots, q, out_h, out_l):
        high, low = halves(jnp.concatenate([slots[2 * q], slots[2 * q + 1]], axis=1))
        both = mm(jnp.concatenate([high, low], axis=0), out_h[q])
        return both[:64] + both[64:] + mm(high, out_l[q])

    def pack(total, dest):
        for pair in range(2):
            top = total[0:32, 128 * pair:128 * pair + 128]
            bottom = total[32:64, 128 * pair:128 * pair + 128]
            dest[2 * pair] = jnp.where(low_lanes, top, pltpu.roll(bottom, 64, 1))
            dest[2 * pair + 1] = jnp.where(low_lanes, pltpu.roll(top, 64, 1), bottom)

    total_a = jnp.zeros((64, 256), F32)
    total_b = jnp.zeros((64, 256), F32)
    for near in ((0,), (2,), (1, 3)):
        for k in near:
            a_all.wait(k)
            b_all.wait(k)
        for k in near:
            total_a = total_a + gradient(sa, lax.rem(x + k, 4), pha_h, pha_l)
            total_b = total_b + gradient(sb, lax.rem(z + k, 4), phb_h, phb_l)
    pack(total_a, ga)
    pack(total_b, gb)
    g_sends = []
    for k in (2, 1, 3):
        send = remote(ga.at[lax.rem(z + k, 4)], gra.at[z], ga_snd.at[k - 1], ga_rcv.at[z], t, zpeer(k))
        send.start()
        g_sends.append(send)
        send = remote(gb.at[lax.rem(x + k, 4)], grb.at[x], gb_snd.at[k - 1], gb_rcv.at[x], t, xpeer(k))
        send.start()
        g_sends.append(send)
    gra[z] = ga[z]
    grb[x] = gb[x]

    for k in range(0, 4):
        for e in range(2):
            if k == 0 and e == 0:
                continue
            d = lax.rem(c + e, 2)
            slot = 2 * lax.rem(x + k, 4) + d
            remote(xr.at[slot], xr.at[slot], x_snd.at[2 * k + e - 1], x_rcv.at[slot], 2 * y + d, xpeer(k)).wait_recv()
    part = xr[0]
    for j in range(1, 8):
        part = part + xr[j]
    xt[...] = part
    for k in range(1, 4):
        send = remote(xt, xz.at[z], x2_snd.at[k - 1], x2_rcv.at[z], t, zpeer(k))
        send.start()
        x_sends.append(send)
    xz[z] = part

    for k in range(1, 8):
        src = tr(k)
        remote(folded.at[0], frows.at[src], f_snd.at[k - 1], f_rcv.at[src], src, sigma).wait_recv()
    remote(sat.at[c], sat.at[1 - c], st_snd, st_rcv, partner, sigma).wait_recv()
    both = jnp.zeros((128, 256), F32)
    for j in range(4):
        left_h, left_l = halves(jnp.concatenate([frows[2 * j], frows[2 * j + 1]], axis=1))
        right = [jnp.concatenate([sat[0, 2 * j + i], sat[1, 2 * j + i]], axis=1) for i in range(2)]
        right_h, right_l = halves(jnp.concatenate(right, axis=0))
        both = both + mm(left_h, right_h) + mm(left_l, right_h) + mm(left_h, right_l)
    feat_out[...] = both

    row = iota((128, 128), 0)
    of_row = (row // 64) * 32 + ((row % 64) // 32) * 64 + row % 32 + 128 * t
    for j in range(16):
        takes = onehot(of_row == sot_ref[:, 128 * j:128 * j + 128])
        memt[0:128, 128 * j:128 * j + 128] = takes
        memt[128:256, 128 * j:128 * j + 128] = takes

    for k in range(1, 4):
        src = lax.rem(z + k, 4)
        remote(ga.at[0], gra.at[src], ga_snd.at[k - 1], ga_rcv.at[src], t, zpeer(k)).wait_recv()
    for k in range(1, 4):
        src = lax.rem(x + k, 4)
        remote(gb.at[0], grb.at[src], gb_snd.at[k - 1], gb_rcv.at[src], t, xpeer(k)).wait_recv()
    grad_a = (gra[0] + gra[1]) + (gra[2] + gra[3])
    grad_b = (grb[0] + grb[1]) + (grb[2] + grb[3])
    grads = jnp.concatenate([grad_a, grad_b], axis=0) * (1.0 / SCEN)
    grads = jnp.concatenate([grads, pltpu.roll(grads, 64, 1)], axis=0).T[0:64, :]
    grads_out[...] = jnp.concatenate(halves(grads), axis=1)

    for k in range(1, 4):
        src = lax.rem(z + k, 4)
        remote(xt, xz.at[src], x2_snd.at[k - 1], x2_rcv.at[src], t, zpeer(k)).wait_recv()
    whole = (xz[0] + xz[1]) + (xz[2] + xz[3])
    first = pl.multiple_of(128 * t, 128)
    xva_out[...] = w_ref[:, pl.ds(first, 128)] * whole[0:1, :] * (1.0 / SCEN)

    for send in party_sends + fac_sends + e_all.sends + f_sends + a_all.sends + b_all.sends + [sat_send] + x_sends + g_sends:
        send.wait_send()


def place_outputs(xva, feat, grads, memt, xva_out, coef_out, feat_out, coef, sem):
    copies = [pltpu.make_async_copy(feat, feat_out, sem.at[4]), pltpu.make_async_copy(xva, xva_out, sem.at[5])]
    for copy in copies:
        copy.start()
    for i in range(4):
        cols = pl.ds(512 * i, 512)
        coef[i] = mm(grads[...], memt[:, 512 * i:512 * i + 512])
        copy = pltpu.make_async_copy(coef.at[i], coef_out.at[:, cols], sem.at[i])
        copy.start()
        copies.append(copy)
    for copy in copies:
        copy.wait()


def local(factors, feat_factor, feat_degree, coefficients, set_of_trade, party_of_set, threshold, weight):
    vmem = pl.BlockSpec(memory_space=pltpu.VMEM)
    hbm = pl.BlockSpec(memory_space=pltpu.HBM)
    V = pltpu.VMEM
    D = pltpu.SemaphoreType.DMA
    scratch = [
        V((1, 1024), jnp.int32), V((1, 1024), jnp.int32), V((1, 2048), jnp.int32),
        V((1, 128), jnp.int32), V((1, 1024), F32), V((1, 1024), F32),
        V((1024, 2048), F32),
        V((2048, 128), BF),
        V((2, 768, 256), BF),
        V((256, 768), BF), V((256, 768), BF),
        V((3, 256, 768), BF), V((3, 256, 768), BF),
        V((4, 64, 256), F32), V((4, 64, 256), F32),
        V((4, 256, 256), BF), V((4, 256, 256), BF), V((4, 256, 256), BF), V((4, 256, 256), BF),
        V((768, 1024), BF),
        V((1024, 256), BF),
        V((8, 128, 128), F32),
        V((8, 128, 128), F32),
        V((2, 128, 128), F32),
        V((8, 128, 128), F32),
        V((1024, 256), BF),
        V((8, 1, 128), jnp.int32),
        V((8, 128, 128), F32),
        V((1024, 1024), BF),
        V((256, 1024), BF),
        V((8, 128, 8), F32),
        V((2, 256, 128), F32),
        V((2, 128, 128), F32),
        V((8, 64, 128), F32), V((8, 64, 128), F32),
        V((2, 8, 128, 128), F32),
        V((2, 8, 128), F32), V((8, 8, 128), F32), V((8, 128), F32), V((4, 8, 128), F32),
        V((4, 32, 128), F32), V((4, 32, 128), F32), V((4, 32, 128), F32), V((4, 32, 128), F32),
        D((8,)), D((8,)), D((7,)), D((8,)), D((3,)), D((4,)), D((3,)), D((4,)), D((14,)), D((16,)), D((7,)), D((8,)),
        D((8,)), D((8,)), D((8,)), D((8,)), D(()), D(()), D((7,)), D((8,)), D((3,)), D((4,)),
        D((3,)), D((4,)), D((3,)), D((4,)),
    ]
    xva_shape = jax.ShapeDtypeStruct((1, 128), F32)
    coef_shape = jax.ShapeDtypeStruct((64, 2048), F32)
    feat_shape = jax.ShapeDtypeStruct((128, 256), F32)
    results = pl.pallas_call(
        kernel,
        out_shape=(xva_shape, feat_shape, jax.ShapeDtypeStruct((64, 256), BF), jax.ShapeDtypeStruct((256, 2048), BF)),
        in_specs=[hbm] * 8,
        out_specs=(vmem, vmem, vmem, vmem),
        scratch_shapes=scratch,
        compiler_params=pltpu.CompilerParams(collective_id=0, has_side_effects=True, vmem_limit_bytes=40 << 20),
    )(*[
        pltpu.with_memory_space_constraint(array, pltpu.HBM)
        for array in (
            coefficients, factors.T, feat_factor.reshape(1, -1), feat_degree.reshape(1, -1),
            set_of_trade.reshape(1, -1), party_of_set.reshape(1, -1), threshold.reshape(1, -1), weight.reshape(1, -1),
        )
    ])
    xva, coef_sens, feature_sens = pl.pallas_call(
        place_outputs,
        out_shape=(xva_shape, coef_shape, feat_shape),
        in_specs=[vmem] * 4,
        out_specs=(hbm, hbm, hbm),
        scratch_shapes=[V((4, 64, 512), F32), D((6,))],
        compiler_params=pltpu.CompilerParams(vmem_limit_bytes=4 << 20),
    )(*results)
    return xva.reshape(-1), coef_sens, feature_sens


def solution(mesh):
    placed = (P("scen", None), P(), P(), P(None, "trade"), P("trade"), P("trade"), P(), P())
    return jax.shard_map(
        local,
        mesh=mesh,
        in_specs=placed,
        out_specs=(P("trade"), P("scen", "trade"), P("trade", "scen")),
        check_vma=False,
    )
```

```python
import jax
import jax.numpy as jnp
from jax import lax
from jax.experimental import pallas as pl
from jax.experimental.pallas import tpu as pltpu
from jax.sharding import PartitionSpec as P

MAXDEG = 12
SCEN = 4096
MESH = pl.DeviceIdType.MESH
BF = jnp.bfloat16
F32 = jnp.float32


def mm(left, right):
    return lax.dot_general(left, right, (((1,), (0,)), ((), ())), preferred_element_type=F32)


def mm_nt(left, right):
    return lax.dot_general(left, right, (((1,), (1,)), ((), ())), preferred_element_type=F32)


def halves(value):
    high = value.astype(BF)
    return high, (value - high.astype(F32)).astype(BF)


def thirds(value):
    high = value.astype(BF)
    rest = value - high.astype(F32)
    mid = rest.astype(BF)
    return high, mid, (rest - mid.astype(F32)).astype(BF)


def iota(shape, dim):
    return lax.broadcasted_iota(jnp.int32, shape, dim)


def onehot(mask):
    return jnp.where(mask, 1.0, 0.0).astype(BF)


def upright(row):
    return jnp.broadcast_to(row, (128, 128)).T


def degree_basis(dup, out_h, out_l):
    low = iota((64, 128), 1) < 64
    for r in range(4):
        rows = slice(64 * r, 64 * r + 64)
        current = dup[rows, :]
        twice = current + current
        before = jnp.ones_like(current)
        for pair in range(MAXDEG // 2):
            after = twice * current - before
            cols = slice(128 * pair, 128 * pair + 128)
            out_h[rows, cols], out_l[rows, cols] = halves(jnp.where(low, current, after))
            if pair < MAXDEG // 2 - 1:
                before, current = after, twice * after - current


def kernel(
    coef_hbm, fac_hbm, ff_hbm, fd_hbm, sot_hbm, pos_hbm, thr_hbm, w_hbm,
    xva_out, feat_out, grads_out, memt,
    ff_ref, fd_ref, sot_ref, pos_ref, thr_ref, w_ref, cbuf,
    member, pick, th, tl, tph, tpl, fax, faz, pha_h, pha_l, phb_h, phb_l,
    spot, fparts, folded, frows, etb, eh, ehl, party, pcol, same, ownp, tw, lims, sas, sa, sb, sat,
    xs, xr, xt, xz, ga, gb, gra, grb, i_sem,
    c_sem, p_snd, p_rcv, fx_snd, fx_rcv, fz_snd, fz_rcv, e_snd, e_rcv, f_snd, f_rcv,
    sa_snd, sa_rcv, sb_snd, sb_rcv, st_snd, st_rcv, x_snd, x_rcv, x2_snd, x2_rcv,
    ga_snd, ga_rcv, gb_snd, gb_rcv,
):
    t = lax.axis_index("trade")
    sigma = lax.axis_index("scen")
    y, c = t // 2, t % 2
    z, x = sigma // 4, sigma % 4
    partner = 2 * y + 1 - c

    def remote(src, dst, snd, rcv, trade, scen):
        return pltpu.make_async_remote_copy(
            src_ref=src, dst_ref=dst, send_sem=snd, recv_sem=rcv,
            device_id=(trade, scen), device_id_type=MESH,
        )

    def tr(k):
        return lax.rem(t + k, 8)

    def xpeer(k):
        return z * 4 + lax.rem(x + k, 4)

    def zpeer(k):
        return lax.rem(z + k, 4) * 4 + x

    class Gather:
        def __init__(self, slots, snd, rcv, mine, place):
            self.slots, self.snd, self.rcv, self.mine, self.place = slots, snd, rcv, mine, place
            self.sends = []

        def put(self, src, slot, i, k, d):
            trade, scen = self.place(k, d)
            send = remote(src, self.slots.at[slot], self.snd.at[i], self.rcv.at[slot], trade, scen)
            send.start()
            self.sends.append(send)

        def start(self, src, e):
            d = lax.rem(c + e, 2)
            for i, k in enumerate((2, 1, 3) + (() if e == 0 else (0,))):
                self.put(src, 2 * self.mine + c, 4 * e + i, k, d)

        def wait(self, k):
            for e in range(2):
                if k or e:
                    slot = 2 * lax.rem(self.mine + k, 4) + lax.rem(c + e, 2)
                    trade, scen = self.place(k, lax.rem(c + e, 2))
                    here = self.slots.at[slot]
                    remote(here, here, self.snd.at[0], self.rcv.at[slot], trade, scen).wait_recv()

    class Relay(Gather):
        def half(self, slot, h):
            return self.slots.at[slot, pl.ds(64 * h, 64)]

        def put(self, src, slot, i, k, d, h):
            trade, scen = self.place(k, d)
            send = remote(src, self.half(slot, h), self.snd.at[i], self.rcv.at[2 * slot + h], trade, scen)
            send.start()
            self.sends.append(send)

        def start(self, src):
            slot = 2 * self.mine + c
            for i, (k, e) in enumerate(((1, 0), (3, 1), (1, 1), (3, 0), (0, 1))):
                d = lax.rem(c + e, 2)
                for h in range(2):
                    self.put(src.at[d, pl.ds(64 * h, 64)], slot, 2 * i + h, k, d, h)

        def wait(self, k, e, h):
            slot = 2 * lax.rem(self.mine + k, 4) + lax.rem(c + e, 2)
            trade, scen = self.place(k if k else 0, lax.rem(c + e, 2))
            here = self.half(slot, h)
            remote(here, here, self.snd.at[0], self.rcv.at[2 * slot + h], trade, scen).wait_recv()
            return slot

        def forward(self):
            for h in range(2):
                slot = self.wait(3, 0, h)
                self.put(self.half(slot, h), slot, 10 + h, 1, c, h)
                slot = self.wait(1, 1, h)
                self.put(self.half(slot, h), slot, 12 + h, 3, c, h)

        def near(self):
            for h in range(2):
                for k, e in ((0, 1), (3, 1), (1, 0)):
                    self.wait(k, e, h)

        def far(self):
            for h in range(2):
                for e in range(2):
                    self.wait(2, e, h)

    smalls = []
    for i, (src, dst) in enumerate((
        (sot_hbm, sot_ref), (ff_hbm, ff_ref), (fd_hbm, fd_ref), (fac_hbm, fax.at[x]), (fac_hbm, faz.at[z]),
        (pos_hbm, pos_ref), (thr_hbm, thr_ref), (w_hbm, w_ref),
    )):
        small = pltpu.make_async_copy(src, dst, i_sem.at[i])
        small.start()
        smalls.append(small)
    loads = []
    for i in range(8):
        rows = pl.ds(128 * i, 128)
        loads.append(pltpu.make_async_copy(coef_hbm.at[rows], cbuf.at[rows], c_sem.at[i]))
    for load in loads:
        load.start(priority=1)
    barrier = pltpu.get_barrier_semaphore()
    for k in range(1, 8):
        pl.semaphore_signal(barrier, inc=1, device_id=(tr(k), sigma), device_id_type=MESH)
    for k in range(1, 4):
        for d in range(2):
            pl.semaphore_signal(barrier, inc=1, device_id=(2 * y + d, xpeer(k)), device_id_type=MESH)
            pl.semaphore_signal(barrier, inc=1, device_id=(2 * y + d, zpeer(k)), device_id_type=MESH)

    for small in smalls:
        small.wait()
    base = (128 * t).astype(F32)
    lanes = iota((128, 128), 1).astype(F32)
    for j in range(16):
        col = upright(sot_ref[:, 128 * j:128 * j + 128].astype(F32) - base)
        member[128 * j:128 * j + 128, :] = onehot(col == lanes)

    def doubled(facts):
        return jnp.concatenate([facts, facts], axis=0).T

    degree_basis(doubled(fax[x]), th, tl)

    keys = (fd_ref[...] - 1) * 64 + ff_ref[...]
    for i in range(8):
        cols = slice(128 * i, 128 * i + 128)
        spot[:, cols] = onehot(iota((768, 128), 0) == keys[:, cols])

    def fold_rows(i):
        rows = slice(256 * i, 256 * i + 256)
        high, low = halves(cbuf[rows, :])
        fold = mm(high, member[...]) + mm(low, member[...])
        folded[2 * i] = fold[:128, :]
        folded[2 * i + 1] = fold[128:, :]
        high, low = halves(fold)
        fparts[rows, 0:128] = high
        fparts[rows, 128:256] = low

    for load in loads[:4]:
        load.wait()
    fold_rows(0)
    fold_rows(1)

    pl.semaphore_wait(barrier, 19)
    party_sends = []
    for k in range(1, 8):
        send = remote(pos_ref, party.at[t], p_snd.at[k - 1], p_rcv.at[t], tr(k), sigma)
        send.start()
        party_sends.append(send)
    fac_sends = []
    for k in range(1, 4):
        send = remote(fax.at[x], fax.at[x], fx_snd.at[k - 1], fx_rcv.at[x], t, xpeer(k))
        send.start()
        fac_sends.append(send)
        send = remote(faz.at[z], faz.at[z], fz_snd.at[k - 1], fz_rcv.at[z], t, zpeer(k))
        send.start()
        fac_sends.append(send)
    party[t] = pos_ref[...]

    for load in loads[4:]:
        load.wait()
    fold_rows(2)
    fold_rows(3)
    wide = mm(spot[...], fparts[...])
    high, low = halves(wide[:, :128] + wide[:, 128:])
    wide = mm(th[...], jnp.concatenate([high, low], axis=1))
    exposure = wide[:, :128] + wide[:, 128:] + mm(tl[...], high)
    etb[0] = exposure[0:128, :].T
    etb[1] = exposure[128:256, :].T

    e_all = Relay(eh, e_snd, e_rcv, y, lambda k, d: (2 * lax.rem(y + k, 4) + d, sigma))
    e_all.start(etb)

    eh[t] = etb[c]
    frows[t] = folded[t]

    for k in range(1, 8):
        src = tr(k)
        remote(pos_ref, party.at[src], p_snd.at[k - 1], p_rcv.at[src], src, sigma).wait_recv()
    for j in range(8):
        pcol[j] = upright(party[j].astype(F32))
    table = thirds(thr_ref[...]) + thirds(w_ref[...])
    table = jnp.concatenate([part.astype(F32) for part in table] + [jnp.zeros((2, 1024), F32)], axis=0).astype(BF)

    def rows_of(j, carry):
        col = pcol[j]
        rows = pl.ds(pl.multiple_of(j * 128, 128), 128)
        for i in range(8):
            same[rows, 128 * i:128 * i + 128] = onehot(col == party[i].astype(F32))
        spread = jnp.concatenate([onehot(col == lanes + 128.0 * i) for i in range(8)], axis=1)
        tw[j] = mm_nt(spread, table)
        return carry

    lax.fori_loop(0, 8, rows_of, 0)

    e_all.forward()

    fvals = jnp.concatenate([ff_ref[...].astype(F32), fd_ref[...].astype(F32), jnp.zeros((6, 1024), F32)], axis=0).astype(BF)
    lane256 = iota((1024, 256), 1)
    fidx_a = ((lane256 // 64) * 4 + x) * 64 + lane256 % 64
    fidx_b = z * 256 + lane256
    for i, fidx in enumerate((fidx_a, fidx_b)):
        picked = mm(fvals, onehot(iota((1024, 256), 0) == fidx)).astype(jnp.int32)
        pick[i] = onehot(iota((768, 256), 0) == (picked[1:2, :] - 1) * 64 + picked[0:1, :])

    def limits(j):
        consts = tw[j]
        return consts[:, 0:1] + consts[:, 1:2] + consts[:, 2:3], consts[:, 3:4] + consts[:, 4:5] + consts[:, 5:6]

    for d in range(2):
        rows = slice(128 * d, 128 * d + 128)
        for i, column in enumerate(limits(2 * y + d)):
            lims[i, rows, :] = jnp.broadcast_to(column, (128, 128))

    def phi_of(buf, which, mine, out_h, out_l):
        out_h[mine] = mm(th[...], pick[which]).astype(BF)
        out_l[mine] = mm(tl[...], pick[which]).astype(BF)
        for k in range(1, 4):
            q = lax.rem(mine + k, 4)
            degree_basis(doubled(buf[q]), tph.at[k - 1], tpl.at[k - 1])
            out_h[q] = mm(tph[k - 1], pick[which]).astype(BF)
            out_l[q] = mm(tpl[k - 1], pick[which]).astype(BF)

    for k in range(1, 4):
        src = lax.rem(x + k, 4)
        remote(fax.at[x], fax.at[src], fx_snd.at[k - 1], fx_rcv.at[src], t, xpeer(k)).wait_recv()
    phi_of(fax, 0, x, pha_h, pha_l)

    def split(m):
        for d in range(2):
            rows = pl.ds(pl.multiple_of(256 * m + 128 * d, 128), 128)
            ehl[rows, 0:128], ehl[rows, 128:256] = halves(eh[2 * m + d])

    chip = pl.ds(pl.multiple_of(256 * y, 256), 256)

    def netted(m):
        cols = pl.ds(pl.multiple_of(256 * m, 256), 256)
        return mm(same[chip, cols], ehl[cols, :])

    e_all.near()
    wide = jnp.zeros((256, 256), F32)
    for k in (0, 1, 3):
        m = lax.rem(y + k, 4)
        split(m)
        wide = wide + netted(m)
    net = wide[:, :128] + wide[:, 128:] - lims[0]
    e_all.far()
    m = lax.rem(y + 2, 4)
    split(m)
    wide = netted(m)
    sas[...] = (lims[1] * jax.nn.sigmoid(net + (wide[:, :128] + wide[:, 128:]))).reshape(2, 128, 128)

    def adjoint(j):
        rows = pl.ds(pl.multiple_of(j * 128, 128), 128)
        wide = mm(same[rows, :], ehl[...])
        shift, scale = limits(j)
        return scale * jax.nn.sigmoid(wide[:, :128] + wide[:, 128:] - shift)

    a_all = Gather(sa, sa_snd, sa_rcv, x, lambda k, d: (2 * y + d, xpeer(k)))
    b_all = Gather(sb, sb_snd, sb_rcv, z, lambda k, d: (2 * y + d, zpeer(k)))
    for e in (1, 0):
        d = lax.rem(c + e, 2)
        a_all.start(sas.at[d, pl.ds(0, 64)], e)
        b_all.start(sas.at[d, pl.ds(64, 64)], e)
    f_sends = []
    for k in (4, 5, 3, 2, 6, 7, 1):
        other = tr(k)
        send = remote(folded.at[other], frows.at[t], f_snd.at[k - 1], f_rcv.at[t], other, sigma)
        send.start()
        f_sends.append(send)
    sa[2 * x + c] = sas[c, 0:64, :]
    sb[2 * z + c] = sas[c, 64:128, :]
    sat[c, 2 * y] = sas[0]
    sat[c, 2 * y + 1] = sas[1]

    for k in range(2, 8):
        j = lax.rem(2 * y + k, 8)
        sat[c, j] = adjoint(j)
    sat_send = remote(sat.at[c], sat.at[c], st_snd, st_rcv, partner, sigma)
    sat_send.start()

    for i in range(8):
        ownp[:, 128 * i:128 * i + 128] = onehot(iota((256, 128), 0) + 256 * y == party[i])
    wide = mm(ownp[...], ehl[...])
    for d in range(2):
        first = pl.multiple_of(256 * y + 128 * d, 128)
        limit = upright(thr_ref[:, pl.ds(first, 128)])
        soft = jax.nn.softplus(wide[128 * d:128 * d + 128, :128] + wide[128 * d:128 * d + 128, 128:] - limit)
        xs[d] = jnp.broadcast_to(jnp.sum(soft.T, axis=0, keepdims=True), (8, 128))
    x_sends = []
    for k in range(0, 4):
        for e in range(2):
            if k == 0 and e == 0:
                continue
            d = lax.rem(c + e, 2)
            send = remote(xs.at[d], xr.at[2 * x + c], x_snd.at[2 * k + e - 1], x_rcv.at[2 * x + c], 2 * y + d, xpeer(k))
            send.start()
            x_sends.append(send)
    xr[2 * x + c] = xs[c]

    for k in range(1, 4):
        src = lax.rem(z + k, 4)
        remote(faz.at[z], faz.at[src], fz_snd.at[k - 1], fz_rcv.at[src], t, zpeer(k)).wait_recv()
    phi_of(faz, 1, z, phb_h, phb_l)

    low_lanes = iota((32, 128), 1) < 64

    def gradient(slots, q, out_h, out_l):
        high, low = halves(jnp.concatenate([slots[2 * q], slots[2 * q + 1]], axis=1))
        both = mm(jnp.concatenate([high, low], axis=0), out_h[q])
        return both[:64] + both[64:] + mm(high, out_l[q])

    def pack(total, dest):
        for pair in range(2):
            top = total[0:32, 128 * pair:128 * pair + 128]
            bottom = total[32:64, 128 * pair:128 * pair + 128]
            dest[2 * pair] = jnp.where(low_lanes, top, pltpu.roll(bottom, 64, 1))
            dest[2 * pair + 1] = jnp.where(low_lanes, pltpu.roll(top, 64, 1), bottom)

    total_a = jnp.zeros((64, 256), F32)
    total_b = jnp.zeros((64, 256), F32)
    def second_sums():
        for k in range(0, 4):
            for e in range(2):
                if k == 0 and e == 0:
                    continue
                d = lax.rem(c + e, 2)
                slot = 2 * lax.rem(x + k, 4) + d
                remote(xr.at[slot], xr.at[slot], x_snd.at[2 * k + e - 1], x_rcv.at[slot], 2 * y + d, xpeer(k)).wait_recv()
        part = xr[0]
        for j in range(1, 8):
            part = part + xr[j]
        xt[...] = part
        for k in range(1, 4):
            send = remote(xt, xz.at[z], x2_snd.at[k - 1], x2_rcv.at[z], t, zpeer(k))
            send.start()
            x_sends.append(send)
        xz[z] = part

    for near in ((0,), (2,), (1, 3)):
        if len(near) > 1:
            second_sums()
        for k in near:
            a_all.wait(k)
            b_all.wait(k)
        for k in near:
            total_a = total_a + gradient(sa, lax.rem(x + k, 4), pha_h, pha_l)
            total_b = total_b + gradient(sb, lax.rem(z + k, 4), phb_h, phb_l)
    pack(total_a, ga)
    pack(total_b, gb)
    g_sends = []
    for k in (2, 1, 3):
        send = remote(ga.at[lax.rem(z + k, 4)], gra.at[z], ga_snd.at[k - 1], ga_rcv.at[z], t, zpeer(k))
        send.start()
        g_sends.append(send)
        send = remote(gb.at[lax.rem(x + k, 4)], grb.at[x], gb_snd.at[k - 1], gb_rcv.at[x], t, xpeer(k))
        send.start()
        g_sends.append(send)
    gra[z] = ga[z]
    grb[x] = gb[x]


    for k in range(1, 8):
        src = tr(k)
        remote(folded.at[0], frows.at[src], f_snd.at[k - 1], f_rcv.at[src], src, sigma).wait_recv()
    remote(sat.at[c], sat.at[1 - c], st_snd, st_rcv, partner, sigma).wait_recv()
    both = jnp.zeros((128, 256), F32)
    for j in range(4):
        left_h, left_l = halves(jnp.concatenate([frows[2 * j], frows[2 * j + 1]], axis=1))
        right = [jnp.concatenate([sat[0, 2 * j + i], sat[1, 2 * j + i]], axis=1) for i in range(2)]
        right_h, right_l = halves(jnp.concatenate(right, axis=0))
        both = both + mm(left_h, right_h) + mm(left_l, right_h) + mm(left_h, right_l)
    feat_out[...] = both

    row = iota((128, 128), 0)
    of_row = (row // 64) * 32 + ((row % 64) // 32) * 64 + row % 32 + 128 * t
    for j in range(16):
        takes = onehot(of_row == sot_ref[:, 128 * j:128 * j + 128])
        memt[0:128, 128 * j:128 * j + 128] = takes
        memt[128:256, 128 * j:128 * j + 128] = takes

    for k in range(1, 4):
        src = lax.rem(z + k, 4)
        remote(ga.at[0], gra.at[src], ga_snd.at[k - 1], ga_rcv.at[src], t, zpeer(k)).wait_recv()
    for k in range(1, 4):
        src = lax.rem(x + k, 4)
        remote(gb.at[0], grb.at[src], gb_snd.at[k - 1], gb_rcv.at[src], t, xpeer(k)).wait_recv()
    grad_a = (gra[0] + gra[1]) + (gra[2] + gra[3])
    grad_b = (grb[0] + grb[1]) + (grb[2] + grb[3])
    grads = jnp.concatenate([grad_a, grad_b], axis=0) * (1.0 / SCEN)
    grads = jnp.concatenate([grads, pltpu.roll(grads, 64, 1)], axis=0).T[0:64, :]
    grads_out[...] = jnp.concatenate(halves(grads), axis=1)

    for k in range(1, 4):
        src = lax.rem(z + k, 4)
        remote(xt, xz.at[src], x2_snd.at[k - 1], x2_rcv.at[src], t, zpeer(k)).wait_recv()
    whole = (xz[0] + xz[1]) + (xz[2] + xz[3])
    first = pl.multiple_of(128 * t, 128)
    xva_out[...] = w_ref[:, pl.ds(first, 128)] * whole[0:1, :] * (1.0 / SCEN)

    for send in party_sends + fac_sends + e_all.sends + f_sends + a_all.sends + b_all.sends + [sat_send] + x_sends + g_sends:
        send.wait_send()


def place_outputs(xva, feat, grads, memt, xva_out, coef_out, feat_out, coef, sem):
    copies = [pltpu.make_async_copy(feat, feat_out, sem.at[4]), pltpu.make_async_copy(xva, xva_out, sem.at[5])]
    for copy in copies:
        copy.start()
    for i in range(4):
        cols = pl.ds(512 * i, 512)
        coef[i] = mm(grads[...], memt[:, 512 * i:512 * i + 512])
        copy = pltpu.make_async_copy(coef.at[i], coef_out.at[:, cols], sem.at[i])
        copy.start()
        copies.append(copy)
    for copy in copies:
        copy.wait()


def local(factors, feat_factor, feat_degree, coefficients, set_of_trade, party_of_set, threshold, weight):
    vmem = pl.BlockSpec(memory_space=pltpu.VMEM)
    hbm = pl.BlockSpec(memory_space=pltpu.HBM)
    V = pltpu.VMEM
    D = pltpu.SemaphoreType.DMA
    scratch = [
        V((1, 1024), jnp.int32), V((1, 1024), jnp.int32), V((1, 2048), jnp.int32),
        V((1, 128), jnp.int32), V((1, 1024), F32), V((1, 1024), F32),
        V((1024, 2048), F32),
        V((2048, 128), BF),
        V((2, 768, 256), BF),
        V((256, 768), BF), V((256, 768), BF),
        V((3, 256, 768), BF), V((3, 256, 768), BF),
        V((4, 64, 256), F32), V((4, 64, 256), F32),
        V((4, 256, 256), BF), V((4, 256, 256), BF), V((4, 256, 256), BF), V((4, 256, 256), BF),
        V((768, 1024), BF),
        V((1024, 256), BF),
        V((8, 128, 128), F32),
        V((8, 128, 128), F32),
        V((2, 128, 128), F32),
        V((8, 128, 128), F32),
        V((1024, 256), BF),
        V((8, 1, 128), jnp.int32),
        V((8, 128, 128), F32),
        V((1024, 1024), BF),
        V((256, 1024), BF),
        V((8, 128, 8), F32),
        V((2, 256, 128), F32),
        V((2, 128, 128), F32),
        V((8, 64, 128), F32), V((8, 64, 128), F32),
        V((2, 8, 128, 128), F32),
        V((2, 8, 128), F32), V((8, 8, 128), F32), V((8, 128), F32), V((4, 8, 128), F32),
        V((4, 32, 128), F32), V((4, 32, 128), F32), V((4, 32, 128), F32), V((4, 32, 128), F32),
        D((8,)), D((8,)), D((7,)), D((8,)), D((3,)), D((4,)), D((3,)), D((4,)), D((14,)), D((16,)), D((7,)), D((8,)),
        D((8,)), D((8,)), D((8,)), D((8,)), D(()), D(()), D((7,)), D((8,)), D((3,)), D((4,)),
        D((3,)), D((4,)), D((3,)), D((4,)),
    ]
    xva_shape = jax.ShapeDtypeStruct((1, 128), F32)
    coef_shape = jax.ShapeDtypeStruct((64, 2048), F32)
    feat_shape = jax.ShapeDtypeStruct((128, 256), F32)
    results = pl.pallas_call(
        kernel,
        out_shape=(xva_shape, feat_shape, jax.ShapeDtypeStruct((64, 256), BF), jax.ShapeDtypeStruct((256, 2048), BF)),
        in_specs=[hbm] * 8,
        out_specs=(vmem, vmem, vmem, vmem),
        scratch_shapes=scratch,
        compiler_params=pltpu.CompilerParams(collective_id=0, has_side_effects=True, vmem_limit_bytes=40 << 20),
    )(*[
        pltpu.with_memory_space_constraint(array, pltpu.HBM)
        for array in (
            coefficients, factors.T, feat_factor.reshape(1, -1), feat_degree.reshape(1, -1),
            set_of_trade.reshape(1, -1), party_of_set.reshape(1, -1), threshold.reshape(1, -1), weight.reshape(1, -1),
        )
    ])
    xva, coef_sens, feature_sens = pl.pallas_call(
        place_outputs,
        out_shape=(xva_shape, coef_shape, feat_shape),
        in_specs=[vmem] * 4,
        out_specs=(hbm, hbm, hbm),
        scratch_shapes=[V((4, 64, 512), F32), D((6,))],
        compiler_params=pltpu.CompilerParams(vmem_limit_bytes=4 << 20),
    )(*results)
    return xva.reshape(-1), coef_sens, feature_sens


def solution(mesh):
    placed = (P("scen", None), P(), P(), P(None, "trade"), P("trade"), P("trade"), P(), P())
    return jax.shard_map(
        local,
        mesh=mesh,
        in_specs=placed,
        out_specs=(P("trade"), P("scen", "trade"), P("trade", "scen")),
        check_vma=False,
    )
```
